128 devices in a mesh: group: 8 (over x, core), tensor: 16 (over y, z).
Axes of the slice: x: 4, y: 4, z: 4, core: 2. Of those that a mesh axis runs over, the one named last changes fastest.
Arguments:
- hidden: bfloat16 [1024, 8192], P('group'), may hold values from -6 to 6
- norm_gain: bfloat16 [8192], replicated, may hold values from 0.5 to 1.5
- query_matrix: bfloat16 [8192, 8192], P(None, 'tensor'), may hold values from -0.0625 to 0.0625
- output_weight: bfloat16 [8192, 8192], P('tensor'), may hold values from -0.0625 to 0.0625
- kv_pages: bfloat16 [1536, 16, 32, 256], P('group', 'tensor'), may hold values from -400 to 400
- page_order: int32 [8, 192], P('group'), may hold values from 0 to 191, each once within a row
- page_counts: int32 [8, 128], P('group'), may hold values from 1 to 8, 192 in all within a row
- page_trims: int32 [8, 128], P('group'), may hold values from 0 to 31
- adapter_store: bfloat16 [64, 8192, 256], P('group', 'tensor'), may hold values from -0.0625 to 0.0625
- store_route: int32 [64, 1], replicated, may hold values from 0 to 7; in each aligned block of 8 rows (0 to 7, 8 to 15, ...) at most 2 rows name the same one
- store_slot: int32 [64], replicated, may hold values from 0 to 7
Outputs:
- layer_out: bfloat16 [1024, 8192], P('group')
The draws below stay inside these ranges and needn't reach their ends.
Inputs may be any that keep to these rules, and one draw needn't show every extreme that they name: `store_route`: in each group's block of 8 segments no store group is named more than 2 times. `page_order`: each group's row names each of its 192 pages once. `page_counts`: each group's counts sum to 192.
All inputs are finite; a program needn't handle non-finite values.
Results may differ from the reference program's by a relative error of at most 0.0092.
Values may be sent and summed in bfloat16 or wider, within the bound.
A program may use at most 128 MiB of HBM per device.

```python
import math
import jax
import jax.numpy as jnp
import numpy as np
from jax import lax

D = 8192
HEADS = 64
KVH = 8
HD = 128
RANK = 64
SEG = 16
HALF = 32
PAGES_MAX = 8
ROWS = 128
ADP_GRP = 8
REQ = 8
CAP = 2
POOL = 192
ADAPTERS = 64
N_GROUP = 8
N_TENSOR = 16


def draw_kv_pages(key, part):
    full_shape = (N_GROUP * POOL, N_TENSOR, HALF, 2 * HD)
    base_key = jax.random.fold_in(key, 11)
    values = jax.random.normal(base_key, full_shape, jnp.float32)
    return jnp.clip(values, -400.0, 400.0).astype(jnp.bfloat16)


def with_ends(values, stream_key, least, largest):
    longest = values.shape.index(max(values.shape))
    spots = []
    for shift in (0, 1):
        where = [jax.random.randint(jax.random.fold_in(stream_key, axis), (), 0, length) for axis, length in enumerate(values.shape)]
        where[longest] = (where[longest] + shift) % values.shape[longest]
        spots.append(tuple(where))
    return values.at[spots[0]].set(least).at[spots[1]].set(largest)


def block_scale(stream_key, shape, cuts, smallest, largest):
    gain, own = 1.0, jax.random.fold_in(stream_key, 6)
    for position, blocks in cuts:
        draws = jnp.exp(jax.random.uniform(jax.random.fold_in(own, position), (blocks,), jnp.float32, smallest / len(cuts), largest / len(cuts)))
        gain = gain * jnp.repeat(draws, shape[position] // blocks).reshape([-1 if axis == position else 1 for axis in range(len(shape))])
    return gain


def profile(amount, total, limit, lean):
    portions = [(1 << 20) // math.isqrt(grade ** lean) + 1 for grade in range(2, amount + 1)]
    surplus, counts = total - limit - (amount - 1), [1] * (amount - 1)
    while surplus > 0:
        movable = [i for i in range(amount - 1) if counts[i] < limit]
        mass, budget = sum([portions[i] for i in movable]), surplus
        for i in movable:
            more = min(limit - counts[i], max(1, budget * portions[i] // mass), surplus)
            counts[i] = counts[i] + more
            surplus = surplus - more
    return np.array([limit] + counts)


def ragged_sizes(key, number_of, total, most, lean):
    if number_of == 2:
        one = jax.random.randint(key, (), max(1, total - most), min(most, total - 1) + 1)
        return jnp.stack([one, total - one])
    tallies = jnp.asarray(profile(number_of, total, most, lean), jnp.int32)
    twos = (number_of - 1) // 2
    source_of, taker = tallies[1:1 + 2 * twos:2], tallies[2:2 + 2 * twos:2]
    room = jnp.minimum(source_of - 1, most - taker)
    shifted = jax.random.randint(jax.random.fold_in(key, 1), (twos,), 0, 1 << 20) % (room + 1)
    tallies = tallies.at[1:1 + 2 * twos:2].set(source_of - shifted).at[2:2 + 2 * twos:2].set(taker + shifted)
    return tallies[jax.random.permutation(jax.random.fold_in(key, 2), number_of)]


def assign_block(stream_key, own, number, rows, amount, top, bound, slope):
    sequence = jax.random.permutation(stream_key, amount)
    heavy_load, ordinary = portions_of(amount, rows * top, bound, slope, True), portions_of(amount, rows * top, bound, slope, False)
    places = jnp.arange(amount)

    def named(sizes, rotation):
        used = int((sizes > 0).sum())
        fixed = max(1, used // 4)
        moved = fixed + (places - fixed + rotation * (used - fixed)) % max(1, amount - fixed)
        return jnp.zeros((amount,), jnp.int32).at[sequence[jnp.where(places < fixed, places, moved)]].set(jnp.asarray(sizes, jnp.int32))

    sizes = jnp.where(number % 4 == 0, named(heavy_load, number // 4), named(ordinary, number - number // 4 - 1))
    mixed = jax.random.permutation(jax.random.fold_in(own, 3), amount)
    giver, sink = mixed[0:amount // 2 * 2:2], mixed[1:amount // 2 * 2:2]
    room = jnp.minimum(sizes[giver] - 1, bound - sizes[sink]) // 2
    room = jnp.where((giver == sequence[0]) | (sink == sequence[0]) | (sizes[sink] == 0), 0, jnp.maximum(room, 0))
    moved = jax.random.randint(jax.random.fold_in(own, 4), (amount // 2,), 0, 1 << 20) % (room + 1)
    sizes = sizes.at[giver].add(-moved).at[sink].add(moved)
    members = jnp.searchsorted(jnp.cumsum(sizes), jnp.arange(rows * top), side="right").astype(jnp.int32)
    listing = members.reshape(top, rows).T
    listing = listing[jax.random.permutation(jax.random.fold_in(own, 1), rows)]
    rotation = jax.random.randint(jax.random.fold_in(own, 2), (rows, 1), 0, top)
    return jnp.take_along_axis(listing, (jnp.arange(top)[None, :] + rotation) % top, axis=1)


def portions_of(number_of, total, most, slope, full):
    portions = [(1 << 20) // math.isqrt(rank ** slope) + 1 for rank in range(1, number_of + 1)]
    largest = most if full else min(most, max(-(-total // number_of), total * portions[0] // sum(portions)))
    least = 1 if total - largest >= number_of - 1 else 0
    given, surplus = [largest] + [least] * (number_of - 1), total - largest - least * (number_of - 1)
    while surplus > 0:
        free = [i for i in range(1, number_of) if given[i] < largest] or [i for i in range(1, number_of) if given[i] < most]
        pool, budget = sum([portions[i] for i in free]), surplus
        for i in free:
            extra = min(most - given[i], max(1, budget * portions[i] // pool), surplus)
            given[i] = given[i] + extra
            surplus = surplus - extra
    return np.array(given)


def normal_values(stream_key, shape, scale, most, cuts=(), held_as=jnp.bfloat16):
    result = jax.random.normal(stream_key, shape, jnp.float32) * scale
    if len(cuts) > 0:
        result = block_scale(stream_key, shape, cuts, -0.22, 0.18) * result
    return jnp.clip(result, min=-most, max=most).astype(held_as)


def setup_inputs(seed: int = 0) -> dict:
    key_list = jax.random.split(jax.random.key(seed), 12)
    hidden = normal_values(key_list[0], (N_GROUP * ROWS, D), 1.0, 6.0, ((0, 8),))
    norm_gain = jnp.clip(1.0 + 0.1 * jax.random.normal(key_list[1], (D,), jnp.float32), 0.5, 1.5).astype(jnp.bfloat16)
    query_matrix = normal_values(key_list[2], (D, D), D ** -0.5, 0.0625, ((1, 16),))
    output_weight = normal_values(key_list[3], (D, D), D ** -0.5, 0.0625, ((0, 16),))
    kv_pages = draw_kv_pages(jax.random.fold_in(key_list[11], 71), 0)
    page_order = jax.vmap(lambda own: jax.random.permutation(own, POOL))(jax.random.split(key_list[5], N_GROUP)).reshape((N_GROUP, POOL)).astype(jnp.int32)
    page_counts = jax.vmap(lambda own: ragged_sizes(own, ROWS, POOL, PAGES_MAX, 2))(jax.random.split(key_list[6], N_GROUP)).reshape((N_GROUP, ROWS)).astype(jnp.int32)
    page_trims = with_ends(jax.random.randint(key_list[7], (N_GROUP, ROWS), 0, HALF), jax.random.fold_in(key_list[7], 1), 0, HALF - 1).astype(jnp.int32)
    adapter_store = normal_values(key_list[8], (ADAPTERS, D, 4 * RANK), D ** -0.5, 0.0625, ((0, 8), (1, 16)))
    store_route_keys = jax.random.split(jax.random.fold_in(key_list[9], 1), (N_GROUP * REQ) // REQ)
    store_route_turns = jax.random.permutation(jax.random.fold_in(key_list[9], 3), (N_GROUP * REQ) // REQ)
    store_route = jax.vmap(lambda own, number: assign_block(jax.random.fold_in(key_list[9], 2), own, number, REQ, N_GROUP, 1, CAP, 2))(store_route_keys, store_route_turns).reshape((N_GROUP * REQ, 1))
    store_slot = with_ends(jax.random.randint(key_list[10], (N_GROUP * REQ,), 0, ADP_GRP), jax.random.fold_in(key_list[10], 1), 0, ADP_GRP - 1).astype(jnp.int32)
    return dict(hidden=hidden, norm_gain=norm_gain, query_matrix=query_matrix, output_weight=output_weight, kv_pages=kv_pages, page_order=page_order, page_counts=page_counts, page_trims=page_trims, adapter_store=adapter_store, store_route=store_route, store_slot=store_slot)


adapter_scale = 2.0
norm_eps = 1e-05
rope_base = 500000.0

def rotate(queries, positions):
    half_dim = queries.shape[-1] // 2
    frequency = rope_base ** (-(jnp.arange(half_dim).astype(jnp.float32) * 2.0) / queries.shape[-1])
    angles = positions[:, None] * frequency[None, :]
    cosine = jnp.cos(angles)[:, None, :]
    sine_table = jnp.sin(angles)[:, None, :]
    lower_part = queries[..., :half_dim]
    upper_part = queries[..., half_dim:]
    return jnp.concatenate([lower_part * cosine - upper_part * sine_table, upper_part * cosine + lower_part * sine_table], axis=-1)

def one_group(group_hidden, group_pages, group_order, group_counts, group_trims, group_route, group_slot, norm_gain, query_matrix, output_weight, adapter_store):
    split_count = N_TENSOR // KVH
    group_heads = HEADS // KVH
    hidden_float32 = group_hidden.astype(jnp.float32)
    inv_rms = lax.rsqrt(lax.optimization_barrier(jnp.mean(hidden_float32 * hidden_float32, axis=1, keepdims=True)) + norm_eps)
    normalized_hidden = (hidden_float32 * inv_rms * norm_gain.astype(jnp.float32)[None, :]).astype(jnp.bfloat16)
    adapter_ids = (group_route * ADP_GRP + group_slot).astype(jnp.int32)
    adapters = adapter_store[adapter_ids].astype(jnp.float32)
    segment_rows = normalized_hidden.astype(jnp.float32).reshape(REQ, SEG, D)
    rank_q = jnp.einsum('ksd,kdr->ksr', segment_rows, adapters[:, :, :RANK]).astype(jnp.bfloat16)
    query_adapter_delta = jnp.einsum('ksr,kdr->ksd', rank_q.astype(jnp.float32), adapters[:, :, 2 * RANK:3 * RANK]).reshape(ROWS, D)
    lengths = (group_counts * split_count * HALF - group_trims).astype(jnp.int32)
    query_float32 = jnp.dot(normalized_hidden, query_matrix, preferred_element_type=jnp.float32) + adapter_scale * query_adapter_delta
    queries = rotate(query_float32.reshape(ROWS, HEADS, HD), (lengths - 1).astype(jnp.float32)).astype(jnp.bfloat16)
    offsets = jnp.cumsum(group_counts) - group_counts
    page_slot = jnp.clip(offsets[:, None] + jnp.arange(PAGES_MAX, dtype=jnp.int32)[None, :], 0, POOL - 1).astype(jnp.int32)
    page_ids = group_order[page_slot]

    def head_block(kv_head):
        head_queries = lax.dynamic_slice_in_dim(queries, kv_head * group_heads, group_heads, 1).astype(jnp.float32)
        maxima = []
        totals = []
        outputs = []
        for part_index in range(split_count):
            column = kv_head * split_count + part_index
            part_cache = lax.dynamic_index_in_dim(group_pages, column, 1, keepdims=False)
            cached = part_cache[page_ids].reshape(ROWS, PAGES_MAX * HALF, 2 * HD).astype(jnp.float32)
            positions = (jnp.arange(PAGES_MAX, dtype=jnp.int32)[:, None] * (split_count * HALF) + part_index * HALF + jnp.arange(HALF, dtype=jnp.int32)[None, :]).reshape(-1)
            usable = positions[None, :] < lengths[:, None]
            scores = jnp.einsum('rgd,rpd->rgp', head_queries, cached[..., :HD]) / math.sqrt(HD)
            masked = jnp.where(usable[:, None, :], scores, -1e+30)
            row_max = lax.optimization_barrier(jnp.max(masked, axis=2))
            weights = jnp.where(usable[:, None, :], jnp.exp(masked - row_max[..., None]), 0.0).astype(jnp.bfloat16)
            totals.append(lax.optimization_barrier(jnp.sum(weights.astype(jnp.float32), axis=2)))
            outputs.append(jnp.einsum('rgp,rpd->rgd', weights.astype(jnp.float32), cached[..., HD:]))
            maxima.append(row_max)
        joint_max = maxima[0]
        for part_index in range(1, split_count):
            joint_max = jnp.maximum(joint_max, maxima[part_index])
        numer = jnp.zeros((ROWS, group_heads, HD), jnp.float32)
        denom = jnp.zeros((ROWS, group_heads), jnp.float32)
        for part_index in range(split_count):
            factor = jnp.exp(maxima[part_index] - joint_max)
            numer = numer + outputs[part_index] * factor[..., None]
            denom = denom + totals[part_index] * factor
        return (numer / denom[..., None]).astype(jnp.bfloat16)
    per_head = lax.map(head_block, jnp.arange(KVH, dtype=jnp.int32))
    attention_result = jnp.moveaxis(per_head, 0, 1).reshape(ROWS, D)
    attended_rows = attention_result.astype(jnp.float32).reshape(REQ, SEG, D)
    rank_o = jnp.einsum('ksd,kdr->ksr', attended_rows, adapters[:, :, RANK:2 * RANK]).astype(jnp.bfloat16)
    output_adapter_delta = jnp.einsum('ksr,kdr->ksd', rank_o.astype(jnp.float32), adapters[:, :, 3 * RANK:]).reshape(ROWS, D)
    projected_rows = jnp.dot(attention_result, output_weight, preferred_element_type=jnp.float32)
    return (hidden_float32 + (projected_rows + adapter_scale * output_adapter_delta)).astype(jnp.bfloat16)

def reference(hidden, norm_gain, query_matrix, output_weight, kv_pages, page_order, page_counts, page_trims, adapter_store, store_route, store_slot):
    stacked = (hidden.reshape(N_GROUP, ROWS, D), kv_pages.reshape(N_GROUP, POOL, N_TENSOR, HALF, 2 * HD), page_order, page_counts, page_trims, store_route.reshape(N_GROUP, REQ), store_slot.reshape(N_GROUP, REQ))

    def per_group(items):
        return one_group(items[0], items[1], items[2], items[3], items[4], items[5], items[6], norm_gain, query_matrix, output_weight, adapter_store)
    layer_out = lax.map(per_group, stacked)
    return layer_out.reshape(N_GROUP * ROWS, D)
```

```python
import functools
import math

import jax
import jax.numpy as jnp
from jax import lax
from jax.experimental import pallas as pl
from jax.experimental.pallas import tpu as pltpu
from jax.sharding import PartitionSpec as P

MESH = pl.DeviceIdType.MESH
F32 = jnp.float32
BF16 = jnp.bfloat16

KVH = 8
HD = 128
SEG = 16
SIDE = 4
NB = 256
adapter_scale = 2.0
norm_eps = 1e-05
rope_base = 500000.0
far_score = -1e30
orders = (2, 1, 3, 0)


def iota(shape, dim):
    return lax.broadcasted_iota(jnp.int32, shape, dim)


def dot(a, b):
    return jnp.dot(a, b, preferred_element_type=F32)


def dot_nt(a, b):
    return lax.dot_general(a, b, (((1,), (1,)), ((), ())), preferred_element_type=F32)


def enter(sizes, g, t):
    groups, tensors = sizes
    barrier = pltpu.get_barrier_semaphore()

    def greet_tensor(d, c):
        pl.semaphore_signal(
            barrier, inc=1, device_id=(g, lax.rem(t + d, tensors)), device_id_type=MESH
        )
        return c

    def greet_group(d, c):
        pl.semaphore_signal(
            barrier, inc=1, device_id=(lax.rem(g + d, groups), t), device_id_type=MESH
        )
        return c

    lax.fori_loop(1, tensors, greet_tensor, 0)
    lax.fori_loop(1, groups, greet_group, 0)
    return lambda: pl.semaphore_wait(barrier, groups + tensors - 2)


def selection(route_ref, slot_ref, g, groups, cap):
    slot_rows = groups * cap * SEG
    segs = groups * 8
    rc = route_ref[pl.ds(pl.multiple_of(g * 8, 8), 8), :].astype(F32)
    lane, sub = iota((8, 128), 1), iota((8, 128), 0)
    own_seg = lane >> 4
    r_row = jnp.sum(jnp.where(own_seg == sub, rc, 0.0), axis=0, keepdims=True)
    rank = jnp.sum(
        jnp.where((rc == r_row) & (sub < own_seg), 1.0, 0.0), axis=0, keepdims=True
    )
    in_seg = (iota((1, 128), 1) & 15).astype(F32)
    spot = (r_row * cap + rank) * SEG + in_seg
    place = jnp.where(iota((slot_rows, 128), 0).astype(F32) == spot, 1.0, 0.0)
    lane, sub = iota((segs, 128), 1), iota((segs, 128), 0)
    mine = jnp.where(route_ref[...] == g, 1.0, 0.0)
    slots = slot_ref[...].astype(F32)
    diag = lane == sub
    mine_row = jnp.sum(jnp.where(diag, mine, 0.0), axis=0, keepdims=True)
    rank = jnp.sum(
        jnp.where(((lane >> 3) == (sub >> 3)) & (lane < sub), mine_row, 0.0),
        axis=1,
        keepdims=True,
    )
    spot = mine * ((iota((segs, 1), 0) >> 3).astype(F32) * cap + rank + 1.0)
    spot_row = jnp.sum(jnp.where(diag, spot, 0.0), axis=0, keepdims=True)
    value_row = jnp.sum(jnp.where(diag, slots + 1.0, 0.0), axis=0, keepdims=True)
    row_slot = (iota((slot_rows, 128), 0) >> 4).astype(F32) + 1.0
    adapter = jnp.sum(jnp.where(spot_row == row_slot, value_row, 0.0), axis=1, keepdims=True) - 1.0
    return place, adapter


class Lora:
    def __init__(self, refs, sizes, g, t, cap):
        (
            self.xs, self.xr, self.ps, self.pr, self.ks, self.ka, self.ds, self.dr,
            self.ssem, self.rsem,
        ) = refs
        self.groups, self.tensors = sizes
        self.g, self.t, self.cap = g, t, cap
        self.rows = cap * SEG

    def pair_copy(self, src, dst, stage, peer, at):
        return pltpu.make_async_remote_copy(
            src_ref=src, dst_ref=dst,
            send_sem=self.ssem.at[stage, peer], recv_sem=self.rsem.at[stage, at],
            device_id=(peer, self.t) if stage % 2 == 0 else (self.g, peer),
            device_id_type=MESH,
        )

    def start(self, src_of, dst, stage):
        me, n = (self.g, self.groups) if stage % 2 == 0 else (self.t, self.tensors)

        def send(d, c):
            peer = lax.rem(me + d, n)
            self.pair_copy(src_of(peer), dst.at[me], stage, peer, me).start()
            return c

        lax.fori_loop(1, n, send, 0)

    def finish(self, src_of, dst, stage):
        me, n = (self.g, self.groups) if stage % 2 == 0 else (self.t, self.tensors)

        def end(d, c):
            peer = lax.rem(me + d, n)
            self.pair_copy(src_of(peer), dst.at[peer], stage, peer, peer).wait()
            return c

        lax.fori_loop(1, n, end, 0)

    def send_rows(self, place, local):
        picked = dot(place.astype(BF16), local).astype(BF16)
        for s in range(self.groups):
            self.xs[s] = picked[s * self.rows : (s + 1) * self.rows]
        self.start(lambda p: self.xs.at[p], self.xr, 0)
        self.xr[self.g] = self.xs[self.g]

    def send_partials(self, adapter, store):
        self.finish(lambda p: self.xs.at[p], self.xr, 0)
        rows = self.xr[...].reshape(self.groups * self.rows, self.xr.shape[2])
        total = jnp.zeros((self.groups * self.rows, 128), F32)
        for pair in range(4):
            factors = jnp.concatenate(
                [store[2 * pair, :, 0:128], store[2 * pair + 1, :, 0:128]], axis=1
            )
            both = dot(rows, factors)
            total = total + jnp.where(adapter == 2.0 * pair, both[:, 0:128], 0.0)
            total = total + jnp.where(adapter == 2.0 * pair + 1.0, both[:, 128:256], 0.0)
        own = total.shape[0] // self.tensors
        for s in range(self.tensors):
            self.ps[s] = total[s * own : (s + 1) * own]
        self.start(lambda p: self.ps.at[p], self.pr, 1)
        self.pr[self.t] = self.ps[self.t]

    def send_ranks(self, first_lane):
        self.finish(lambda p: self.ps.at[p], self.pr, 1)
        total = self.pr[0]
        for s in range(1, self.tensors):
            total = total + self.pr[s]
        lane = iota(total.shape, 1)
        total = jnp.where((lane >= first_lane) & (lane < first_lane + 64), total, 0.0)
        self.ks[...] = total.astype(BF16)
        self.start(lambda p: self.ks, self.ka, 3)
        self.ka[self.t] = self.ks[...]

    def send_updates(self, adapter, store):
        self.finish(lambda p: self.ks, self.ka, 3)
        rank = self.ka[...].reshape(self.groups * self.rows, 128).astype(F32)
        total = None
        for pair in range(4):
            low = jnp.concatenate(
                [
                    jnp.where(adapter == 2.0 * pair, rank, 0.0),
                    jnp.where(adapter == 2.0 * pair + 1.0, rank, 0.0),
                ],
                axis=1,
            ).astype(BF16)
            factors = jnp.concatenate(
                [store[2 * pair, :, 128:256], store[2 * pair + 1, :, 128:256]], axis=1
            )
            part = dot_nt(low, factors)
            total = part if total is None else total + part
        total = total.astype(BF16)
        for s in range(self.groups):
            self.ds[s] = total[s * self.rows : (s + 1) * self.rows]
        self.start(lambda p: self.ds.at[p], self.dr, 2)
        self.dr[self.g] = self.ds[self.g]

    def update(self, place):
        self.finish(lambda p: self.ds.at[p], self.dr, 2)
        rows = self.dr[...].reshape(self.groups * self.rows, self.dr.shape[2])
        return adapter_scale * dot(place.T.astype(BF16), rows)


def lora_scratch(sizes, cap, width):
    groups, tensors = sizes
    own = groups * cap * SEG // tensors
    big = max(groups, tensors)
    return [
        pltpu.VMEM((groups, cap * SEG, width), BF16),
        pltpu.VMEM((groups, cap * SEG, width), BF16),
        pltpu.VMEM((tensors, own, 128), F32),
        pltpu.VMEM((tensors, own, 128), F32),
        pltpu.VMEM((own, 128), BF16),
        pltpu.VMEM((tensors, own, 128), BF16),
        pltpu.VMEM((groups, cap * SEG, width), BF16),
        pltpu.VMEM((groups, cap * SEG, width), BF16),
        pltpu.SemaphoreType.DMA((4, big)),
        pltpu.SemaphoreType.DMA((4, big)),
    ]


def query_kernel(
    sizes, cap,
    gain_ref, cos_ref, sin_ref, route_ref, slot_ref, hidden_hbm, matrix_hbm, store_hbm,
    q_ref,
    hidden_ref, normed_ref, matrix_ref, store_ref, inv_ref, acc_ref, load_sem, pair_sem,
    *lora_refs,
):
    g, t = lax.axis_index("group"), lax.axis_index("tensor")
    chunks = matrix_ref.shape[0]
    depth = matrix_ref.shape[1]
    rows, width = hidden_ref.shape
    local_width = matrix_ref.shape[2]
    hidden_load = pltpu.make_async_copy(hidden_hbm, hidden_ref, load_sem.at[chunks])
    hidden_load.start()
    loads = [
        pltpu.make_async_copy(
            matrix_hbm.at[pl.ds(k * depth, depth), :], matrix_ref.at[k], load_sem.at[k]
        )
        for k in range(chunks)
    ]
    store_load = pltpu.make_async_copy(store_hbm, store_ref, load_sem.at[chunks + 1])
    for k in range(2):
        loads[k].start()
    store_load.start()
    for k in range(2, chunks):
        loads[k].start()
    all_in = enter(sizes, g, t)
    place, adapter = selection(route_ref, slot_ref, g, sizes[0], cap)
    lora = Lora(lora_refs, sizes, g, t, cap)
    hidden_load.wait()

    def squares(r, c):
        at = pl.ds(pl.multiple_of(r * 16, 16), 16)
        total = jnp.zeros((16, 128), F32)
        for k in range(width // 1024):
            x = hidden_ref[at, k * 1024 : (k + 1) * 1024].astype(F32)
            x = x * x
            for j in range(8):
                total = total + x[:, j * 128 : (j + 1) * 128]
        mean = jnp.sum(total, axis=1, keepdims=True) / width
        inv_ref[at, :] = jnp.broadcast_to(lax.rsqrt(mean + norm_eps), (16, 128))
        return c

    lax.fori_loop(0, rows // 16, squares, 0)
    own_cols = pl.ds(pl.multiple_of(t * local_width, local_width), local_width)
    local = (
        hidden_ref[:, own_cols].astype(F32) * inv_ref[:, 0:1] * gain_ref[:, own_cols].astype(F32)
    ).astype(BF16)
    all_in()
    lora.send_rows(place, local)

    def normalize(r, c):
        at = pl.ds(pl.multiple_of(r * 16, 16), 16)
        inv = inv_ref[at, 0:1]
        for k in range(width // 1024):
            cols = slice(k * 1024, (k + 1) * 1024)
            normed_ref[at, cols] = (
                hidden_ref[at, cols].astype(F32) * inv * gain_ref[:, cols].astype(F32)
            ).astype(BF16)
        return c

    lax.fori_loop(0, rows // 16, normalize, 0)

    def project(k):
        loads[k].wait()
        part = dot(normed_ref[:, k * depth : (k + 1) * depth], matrix_ref[k])
        acc_ref[...] = part if k == 0 else acc_ref[...] + part

    for k in range(4):
        project(k)
    store_load.wait()
    lora.send_partials(adapter, store_ref)
    for k in range(4, chunks):
        project(k)
    lora.send_ranks(0)
    lora.send_updates(adapter, store_ref)
    full = acc_ref[...] + lora.update(place)
    part = lax.rem(t, 2)
    heads = []
    for h in range(local_width // HD):
        x = full[:, h * HD : (h + 1) * HD]
        heads.append(x * cos_ref[...] + pltpu.roll(x, HD // 2, 1) * sin_ref[...])
    own_half = pl.ds(pl.multiple_of(part * local_width, local_width), local_width)
    q_ref[:, own_half] = jnp.concatenate(heads, axis=1).astype(BF16)
    other_half = pl.ds(pl.multiple_of((1 - part) * local_width, local_width), local_width)
    partner = t + 1 - 2 * part
    send = pltpu.make_async_remote_copy(
        src_ref=q_ref.at[:, own_half], dst_ref=q_ref.at[:, own_half],
        send_sem=pair_sem.at[0], recv_sem=pair_sem.at[1],
        device_id=(g, partner), device_id_type=MESH,
    )
    send.start()
    send.wait_send()
    pltpu.make_async_remote_copy(
        src_ref=q_ref.at[:, other_half], dst_ref=q_ref.at[:, other_half],
        send_sem=pair_sem.at[0], recv_sem=pair_sem.at[1],
        device_id=(g, partner), device_id_type=MESH,
    ).wait_recv()


def attend(q, kv_ref, order_ref, counts_ref, trims_ref, part, o_ref, ml_ref, work):
    own_ref, qp_ref, op_ref, mp_ref, lp_ref = work
    rows = counts_ref.shape[1]
    pool = order_ref.shape[1]
    heads = q.shape[1] // HD
    half = kv_ref.shape[0] // pool
    block = NB // half
    counts = counts_ref[...].astype(F32)
    trims = trims_ref[...].astype(F32)
    square = (rows, rows)
    diag = iota(square, 0) == iota(square, 1)
    count_col = jnp.sum(jnp.where(diag, counts, 0.0), axis=1, keepdims=True)
    offsets = jnp.sum(
        jnp.where(iota(square, 0) < iota(square, 1), count_col, 0.0), axis=0, keepdims=True
    )
    lengths = counts * (2 * half) - trims
    spot = jnp.sum(
        jnp.where(order_ref[...] == iota((pool, pool), 0), iota((pool, pool), 1).astype(F32), 0.0),
        axis=1,
        keepdims=True,
    )
    owner = (spot >= offsets) & (spot < offsets + counts)
    own_ref[...] = jnp.where(owner, 1.0, 0.0)
    first = (part * half).astype(F32)
    used = jnp.sum(
        jnp.where(owner, lengths - (spot - offsets) * (2 * half) - first, 0.0),
        axis=1,
        keepdims=True,
    )
    qp_ref[...] = dot(own_ref[...].astype(BF16), q)
    wide = (block * heads, NB)
    same_page = (iota(wide, 1) // half) == (iota(wide, 0) & (block - 1))
    slot = (iota(wide, 1) & (half - 1)).astype(F32)
    for b in range(pool // block):
        pages = slice(b * block, (b + 1) * block)
        query = jnp.concatenate(
            [qp_ref[pages, h * HD : (h + 1) * HD] for h in range(heads)], axis=0
        ).astype(BF16)
        keys = kv_ref[b * NB : (b + 1) * NB, 0:HD]
        values = kv_ref[b * NB : (b + 1) * NB, HD : 2 * HD]
        scores = dot_nt(query, keys) / math.sqrt(HD)
        limit = jnp.concatenate([used[pages]] * heads, axis=0)
        usable = same_page & (slot < limit)
        masked = jnp.where(usable, scores, far_score)
        top = jnp.max(masked, axis=1, keepdims=True)
        weights = jnp.where(usable, jnp.exp(masked - top), 0.0).astype(BF16)
        total = jnp.sum(weights.astype(F32), axis=1, keepdims=True)
        op_ref[b] = dot(weights, values)
        mp_ref[b] = jnp.broadcast_to(top, (block * heads, HD))
        lp_ref[b] = jnp.broadcast_to(total, (block * heads, HD))
    own_t = own_ref[...].T.astype(BF16)
    lane = iota((rows, HD), 1)
    summary = jnp.zeros((rows, HD), F32)
    for h in range(heads):
        inner = slice(h * block, (h + 1) * block)
        top = jnp.full((block, rows), far_score, F32)
        for b in range(pool // block):
            mine = own_ref[b * block : (b + 1) * block, :] > 0.0
            top = jnp.maximum(top, jnp.where(mine, mp_ref[b, inner, :], far_score))
        top = jnp.max(top, axis=0, keepdims=True)
        total = jnp.zeros((block, rows), F32)
        scaled = []
        for b in range(pool // block):
            mine = own_ref[b * block : (b + 1) * block, :] > 0.0
            page_top = jnp.max(jnp.where(mine, top, far_score), axis=1, keepdims=True)
            factor = jnp.exp(mp_ref[b, inner, :] - page_top)
            scaled.append(op_ref[b, inner, :] * factor)
            total = total + jnp.where(mine, lp_ref[b, inner, :] * factor, 0.0)
        total = jnp.sum(total, axis=0, keepdims=True)
        o_ref[:, h * HD : (h + 1) * HD] = dot(own_t, jnp.concatenate(scaled, axis=0).astype(BF16))
        top_col = jnp.sum(jnp.where(diag, top, 0.0), axis=1, keepdims=True)
        total_col = jnp.sum(jnp.where(diag, total, 0.0), axis=1, keepdims=True)
        summary = jnp.where(lane == h, top_col, summary)
        summary = jnp.where(lane == heads + h, total_col, summary)
    ml_ref[...] = summary


class Torus:
    def __init__(self, g, t):
        self.g, self.y, self.z = g, t // SIDE, lax.rem(t, SIDE)

    def at(self, h, da, db):
        dy, dz = (da, db) if h == 0 else (db, da)
        return lax.rem(self.y + dy, SIDE) * SIDE + lax.rem(self.z + dz, SIDE)

    def near(self, h, level, sign):
        step = 1 if sign > 0 else SIDE - 1
        return (self.g, self.at(h, step, 0) if level < 4 else self.at(h, 0, step))


def output_kernel(
    sizes, cap,
    q_ref, order_ref, counts_ref, trims_ref, route_ref, slot_ref,
    kv_hbm, weight_hbm, hidden_hbm, store_hbm,
    out_ref,
    kv_ref, weight_ref, hidden_ref, store_ref, o_ref, ml_ref,
    own_ref, qp_ref, op_ref, mp_ref, lp_ref,
    os_ref, or_ref, mr_ref, att_ref, snd, rcv, keep, mine, fin,
    load_sem, pair_sem, rs_s, rs_r, ag_s, ag_r,
    *lora_refs,
):
    g, t = lax.axis_index("group"), lax.axis_index("tensor")
    part = lax.rem(t, 2)
    partner = t + 1 - 2 * part
    width = att_ref.shape[1]
    own_cols = pl.ds(pl.multiple_of(t * width, width), width)
    loads = [
        pltpu.make_async_copy(kv_hbm, kv_ref, load_sem.at[0]),
        pltpu.make_async_copy(weight_hbm, weight_ref, load_sem.at[1]),
        pltpu.make_async_copy(store_hbm, store_ref, load_sem.at[2]),
        pltpu.make_async_copy(hidden_hbm.at[:, own_cols], hidden_ref, load_sem.at[3]),
    ]
    for load in loads:
        load.start()
    all_in = enter(sizes, g, t)
    place, adapter = selection(route_ref, slot_ref, g, sizes[0], cap)
    lora = Lora(lora_refs, sizes, g, t, cap)
    torus = Torus(g, t)
    loads[0].wait()
    attend(
        q_ref[...], kv_ref, order_ref, counts_ref, trims_ref, part, o_ref, ml_ref,
        (own_ref, qp_ref, op_ref, mp_ref, lp_ref),
    )
    all_in()

    own_half = pl.ds(pl.multiple_of(part * width, width), width)
    other_half = pl.ds(pl.multiple_of((1 - part) * width, width), width)
    os_ref[...] = o_ref[:, other_half].astype(BF16)
    pair = [
        pltpu.make_async_remote_copy(
            src_ref=src, dst_ref=dst, send_sem=pair_sem.at[0, i], recv_sem=pair_sem.at[1, i],
            device_id=(g, partner), device_id_type=MESH,
        )
        for i, (src, dst) in enumerate(((ml_ref, mr_ref), (os_ref, or_ref)))
    ]
    for copy in pair:
        copy.start()
    for copy in pair:
        copy.wait()
    lane = iota(ml_ref.shape, 1)
    for i in range(width // HD):
        cols = slice(i * HD, (i + 1) * HD)
        head = part * (width // HD) + i

        def pick(ref, first):
            return jnp.sum(jnp.where(lane == head + first, ref[...], 0.0), axis=1, keepdims=True)

        own_top, other_top = pick(ml_ref, 0), pick(mr_ref, 0)
        top = jnp.maximum(own_top, other_top)
        own_scale, other_scale = jnp.exp(own_top - top), jnp.exp(other_top - top)
        total = pick(ml_ref, 8) * own_scale + pick(mr_ref, 8) * other_scale
        own_o = o_ref[:, pl.ds(pl.multiple_of(part * width + i * HD, HD), HD)]
        joined = own_o * own_scale + or_ref[:, cols].astype(F32) * other_scale
        att_ref[:, cols] = (joined / total).astype(BF16)

    lora.send_rows(place, att_ref[...])

    def block(h, da, db):
        col = torus.at(h, da, db) * (2 * NB) + h * NB
        return dot(att_ref[...], weight_ref[:, pl.ds(pl.multiple_of(col, NB), NB)])

    def copy_of(h, level, kind):
        return pltpu.make_async_remote_copy(
            src_ref=snd.at[h, level, kind], dst_ref=rcv.at[h, level, kind],
            send_sem=rs_s.at[h, level, kind], recv_sem=rs_r.at[h, level, kind],
            device_id=torus.near(h, level, 1 if kind % 2 == 0 else -1), device_id_type=MESH,
        )

    def send(h, level, kind, value):
        snd[h, level, kind] = value.astype(BF16)
        copy_of(h, level, kind).start()

    def got(h, level, kind):
        copy_of(h, level, kind).wait_recv()
        return rcv[h, level, kind].astype(F32)

    def send_far(h, level, value):
        send(h, level, 0, value[:64])
        send(h, level, 1, value[64:])

    def send_plus(h, level, value):
        send(h, level, 2, value[64:])
        keep[h, level, 0] = value[:64]

    def send_minus(h, level, value):
        send(h, level, 3, value[:64])
        keep[h, level, 1] = value[64:]

    def relay(h, level):
        send(h, level, 4, keep[h, level, 0] + got(h, level, 0))
        send(h, level, 5, keep[h, level, 1] + got(h, level, 1))

    def arrived(h, level, value):
        upper = value[:64] + got(h, level, 3) + got(h, level, 4)
        lower = value[64:] + got(h, level, 2) + got(h, level, 5)
        return jnp.concatenate([upper, lower], axis=0)

    loads[1].wait()
    for level, db in enumerate(orders):
        for h in range(2):
            send_far(h, level, block(h, 2, db))
    for level, db in enumerate(orders):
        for h in range(2):
            send_plus(h, level, block(h, 1, db))
            send_minus(h, level, block(h, 3, db))
    loads[2].wait()
    lora.send_partials(adapter, store_ref)
    for level, db in enumerate(orders):
        for h in range(2):
            mine[h, level] = block(h, 0, db)
    for level in range(4):
        for h in range(2):
            relay(h, level)
    lora.send_ranks(64)
    for level in range(4):
        for h in range(2):
            value = arrived(h, level, mine[h, level])
            if level == 0:
                send_far(h, 4, value)
            elif level == 1:
                send_plus(h, 4, value)
            elif level == 2:
                send_minus(h, 4, value)
            else:
                fin[h] = value
    lora.send_updates(adapter, store_ref)
    for h in range(2):
        relay(h, 4)
    loads[3].wait()
    update = lora.update(place)
    for h in range(2):
        cols = slice(h * NB, (h + 1) * NB)
        total = arrived(h, 4, fin[h]) + update[:, cols] + hidden_ref[:, cols].astype(F32)
        col = t * width + h * NB
        out_ref[:, pl.ds(pl.multiple_of(col, NB), NB)] = total.astype(BF16)

    def spread(h, level, kind, da, db):
        col = torus.at(h, da, db) * (2 * NB) + h * NB
        rows = (slice(0, 128), slice(0, 128), slice(0, 64), slice(64, 128))[kind]
        place_at = out_ref.at[rows, pl.ds(pl.multiple_of(col, NB), NB)]
        return pltpu.make_async_remote_copy(
            src_ref=place_at, dst_ref=place_at,
            send_sem=ag_s.at[h, level, kind], recv_sem=ag_r.at[h, level, kind],
            device_id=torus.near(h, level, 1 if kind % 2 == 0 else -1), device_id_type=MESH,
        )

    sent = (0, 0, 3, 1)
    brought = (3, 1, 2, 2)

    def go(h, level, kind):
        if level == 4:
            spread(h, level, kind, 0, sent[kind]).start()
        else:
            spread(h, level, kind, sent[kind], level).start()

    def came(h, level, kind):
        if level == 4:
            spread(h, level, kind, 0, brought[kind]).wait_recv()
        else:
            spread(h, level, kind, brought[kind], level).wait_recv()

    def left(h, level, kind):
        if level == 4:
            spread(h, level, kind, 0, sent[kind]).wait_send()
        else:
            spread(h, level, kind, sent[kind], level).wait_send()

    def go_both(h, level):
        go(h, level, 0)
        go(h, level, 1)

    def pass_on(h, level):
        came(h, level, 0)
        go(h, level, 2)
        came(h, level, 1)
        go(h, level, 3)

    for h in range(2):
        go_both(h, 4)
    for h in range(2):
        go_both(h, 0)
    for h in range(2):
        came(h, 4, 0)
        go(h, 4, 2)
        go_both(h, 3)
        came(h, 4, 1)
        go(h, 4, 3)
        go_both(h, 1)
    for h in range(2):
        pass_on(h, 0)
    for h in range(2):
        came(h, 4, 2)
        came(h, 4, 3)
        go_both(h, 2)
    for level in (3, 1, 2):
        for h in range(2):
            pass_on(h, level)
    for level in (0, 3, 1, 2):
        for h in range(2):
            came(h, level, 2)
            came(h, level, 3)
    for level in range(5):
        for h in range(2):
            for kind in range(6):
                copy_of(h, level, kind).wait_send()
            for kind in range(4):
                left(h, level, kind)


def body(
    sizes,
    hidden, norm_gain, query_matrix, output_weight, kv_pages, page_order, page_counts,
    page_trims, adapter_store, store_route, store_slot,
):
    groups = sizes[0]
    cap = max(2, 16 // groups) if groups > 1 else 8
    rows, width = hidden.shape
    local_width = query_matrix.shape[1]
    pool, _, half, lanes = kv_pages.shape
    stored = adapter_store.shape[0]
    slots = store_slot.reshape(-1, 1)
    lengths = page_counts[0] * (2 * half) - page_trims[0]
    half_dim = HD // 2
    frequency = rope_base ** (-(jnp.arange(half_dim).astype(F32) * 2.0) / HD)
    angles = (lengths - 1).astype(F32)[:, None] * frequency[None, :]
    cosine, sine = jnp.cos(angles), jnp.sin(angles)
    cos_table = jnp.concatenate([cosine, cosine], axis=1)
    sin_table = jnp.concatenate([-sine, sine], axis=1)
    vmem = pl.BlockSpec(memory_space=pltpu.VMEM)
    anywhere = pl.BlockSpec(memory_space=pl.ANY)
    chunks = 8
    query = pl.pallas_call(
        functools.partial(query_kernel, sizes, cap),
        out_shape=jax.ShapeDtypeStruct((rows, 2 * local_width), BF16),
        in_specs=[vmem] * 5 + [anywhere] * 3,
        out_specs=vmem,
        scratch_shapes=[
            pltpu.VMEM((rows, width), BF16),
            pltpu.VMEM((rows, width), BF16),
            pltpu.VMEM((chunks, width // chunks, local_width), BF16),
            pltpu.VMEM((stored, local_width, lanes), BF16),
            pltpu.VMEM((rows, 128), F32),
            pltpu.VMEM((rows, local_width), F32),
            pltpu.SemaphoreType.DMA((chunks + 2,)),
            pltpu.SemaphoreType.DMA((2,)),
        ]
        + lora_scratch(sizes, cap, local_width),
        compiler_params=pltpu.CompilerParams(
            collective_id=0, has_side_effects=True, vmem_limit_bytes=48 << 20
        ),
        name="query_part",
    )(
        norm_gain.reshape(1, -1), cos_table, sin_table, store_route, slots,
        hidden, query_matrix, adapter_store,
    )
    blocks = pool * half // NB
    block_rows = (NB // half) * (2 * local_width // HD)
    return pl.pallas_call(
        functools.partial(output_kernel, sizes, cap),
        out_shape=jax.ShapeDtypeStruct((rows, width), BF16),
        in_specs=[vmem] * 6 + [anywhere] * 4,
        out_specs=vmem,
        scratch_shapes=[
            pltpu.VMEM((pool * half, lanes), BF16),
            pltpu.VMEM((local_width, width), BF16),
            pltpu.VMEM((rows, local_width), BF16),
            pltpu.VMEM((stored, local_width, lanes), BF16),
            pltpu.VMEM((rows, 2 * local_width), F32),
            pltpu.VMEM((rows, 128), F32),
            pltpu.VMEM((pool, rows), F32),
            pltpu.VMEM((pool, 2 * local_width), F32),
            pltpu.VMEM((blocks, block_rows, HD), F32),
            pltpu.VMEM((blocks, block_rows, HD), F32),
            pltpu.VMEM((blocks, block_rows, HD), F32),
            pltpu.VMEM((rows, local_width), BF16),
            pltpu.VMEM((rows, local_width), BF16),
            pltpu.VMEM((rows, 128), F32),
            pltpu.VMEM((rows, local_width), BF16),
            pltpu.VMEM((2, 5, 6, rows // 2, NB), BF16),
            pltpu.VMEM((2, 5, 6, rows // 2, NB), BF16),
            pltpu.VMEM((2, 5, 2, rows // 2, NB), F32),
            pltpu.VMEM((2, 4, rows, NB), F32),
            pltpu.VMEM((2, rows, NB), F32),
            pltpu.SemaphoreType.DMA((4,)),
            pltpu.SemaphoreType.DMA((2, 2)),
            pltpu.SemaphoreType.DMA((2, 5, 6)),
            pltpu.SemaphoreType.DMA((2, 5, 6)),
            pltpu.SemaphoreType.DMA((2, 5, 4)),
            pltpu.SemaphoreType.DMA((2, 5, 4)),
        ]
        + lora_scratch(sizes, cap, local_width),
        compiler_params=pltpu.CompilerParams(
            collective_id=1, has_side_effects=True, vmem_limit_bytes=48 << 20
        ),
        name="output_part",
    )(
        query, page_order, page_counts, page_trims, store_route, slots,
        kv_pages.reshape(pool * half, lanes), output_weight, hidden, adapter_store,
    )


def solution(mesh):
    sizes = (mesh.shape["group"], mesh.shape["tensor"])
    in_specs = (
        P("group", None),
        P(),
        P(None, "tensor"),
        P("tensor", None),
        P("group", "tensor", None, None),
        P("group", None),
        P("group", None),
        P("group", None),
        P("group", "tensor", None),
        P(),
        P(),
    )
    return jax.shard_map(
        functools.partial(body, sizes),
        mesh=mesh,
        in_specs=in_specs,
        out_specs=P("group", None),
        check_vma=False,
    )
```

```python
import functools
import math

import jax
import jax.numpy as jnp
from jax import lax
from jax.experimental import pallas as pl
from jax.experimental.pallas import tpu as pltpu
from jax.sharding import PartitionSpec as P

MESH = pl.DeviceIdType.MESH
F32 = jnp.float32
BF16 = jnp.bfloat16

KVH = 8
HD = 128
SEG = 16
SIDE = 4
NB = 256
adapter_scale = 2.0
norm_eps = 1e-05
rope_base = 500000.0
far_score = -1e30
orders = (2, 1, 3, 0)


def iota(shape, dim):
    return lax.broadcasted_iota(jnp.int32, shape, dim)


def dot(a, b):
    return jnp.dot(a, b, preferred_element_type=F32)


def dot_nt(a, b):
    return lax.dot_general(a, b, (((1,), (1,)), ((), ())), preferred_element_type=F32)


def enter(sizes, g, t):
    groups, tensors = sizes
    barrier = pltpu.get_barrier_semaphore()

    def greet_tensor(d, c):
        pl.semaphore_signal(
            barrier, inc=1, device_id=(g, lax.rem(t + d, tensors)), device_id_type=MESH
        )
        return c

    def greet_group(d, c):
        pl.semaphore_signal(
            barrier, inc=1, device_id=(lax.rem(g + d, groups), t), device_id_type=MESH
        )
        return c

    lax.fori_loop(1, tensors, greet_tensor, 0)
    lax.fori_loop(1, groups, greet_group, 0)
    return lambda: pl.semaphore_wait(barrier, groups + tensors - 2)


def selection(route_row, slots, g, groups, cap):
    slot_rows = groups * cap * SEG
    segs = groups * 8
    value_row = slots + 1.0
    lane, sub = iota((segs, segs), 1), iota((segs, segs), 0)
    diag = lane == sub
    route_col = jnp.sum(jnp.where(diag, route_row, 0.0), axis=1, keepdims=True)
    me = g.astype(F32)
    mine = jnp.where(route_col == me, 1.0, 0.0)
    mine_row = jnp.where(route_row == me, 1.0, 0.0)
    rank = jnp.sum(
        jnp.where(((lane >> 3) == (sub >> 3)) & (lane < sub), mine_row, 0.0),
        axis=1,
        keepdims=True,
    )
    spot = mine * ((iota((segs, 1), 0) >> 3).astype(F32) * cap + rank + 1.0)
    spot_row = jnp.sum(jnp.where(diag, spot, 0.0), axis=0, keepdims=True)
    row_slot = (iota((slot_rows, segs), 0) >> 4).astype(F32) + 1.0
    adapter = jnp.sum(jnp.where(spot_row == row_slot, value_row, 0.0), axis=1, keepdims=True) - 1.0
    lane, sub = iota((segs, 128), 1), iota((segs, 128), 0)
    own_seg = lane >> 4
    in_group = (sub >> 3) == g
    r_row = jnp.sum(
        jnp.where(in_group & (own_seg == (sub & 7)), route_col, 0.0), axis=0, keepdims=True
    )
    rank = jnp.sum(
        jnp.where(in_group & (route_col == r_row) & ((sub & 7) < own_seg), 1.0, 0.0),
        axis=0,
        keepdims=True,
    )
    in_seg = (iota((1, 128), 1) & 15).astype(F32)
    spot = (r_row * cap + rank) * SEG + in_seg
    place = jnp.where(iota((slot_rows, 128), 0).astype(F32) == spot, 1.0, 0.0)
    return place, adapter


class Lora:
    def __init__(self, refs, sizes, g, t, cap):
        (
            self.xs, self.xr, self.ps, self.pr, self.ks, self.ka, self.ds, self.dr,
            self.ssem, self.rsem,
        ) = refs
        self.groups, self.tensors = sizes
        self.g, self.t, self.cap = g, t, cap
        self.rows = cap * SEG

    def pair_copy(self, src, dst, stage, peer, at):
        return pltpu.make_async_remote_copy(
            src_ref=src, dst_ref=dst,
            send_sem=self.ssem.at[stage, peer], recv_sem=self.rsem.at[stage, at],
            device_id=(peer, self.t) if stage % 2 == 0 else (self.g, peer),
            device_id_type=MESH,
        )

    def start(self, src_of, dst, stage):
        me, n = (self.g, self.groups) if stage % 2 == 0 else (self.t, self.tensors)

        def send(d, c):
            peer = lax.rem(me + d, n)
            self.pair_copy(src_of(peer), dst.at[me], stage, peer, me).start()
            return c

        lax.fori_loop(1, n, send, 0)

    def finish(self, src_of, dst, stage):
        me, n = (self.g, self.groups) if stage % 2 == 0 else (self.t, self.tensors)

        def end(d, c):
            peer = lax.rem(me + d, n)
            self.pair_copy(src_of(peer), dst.at[peer], stage, peer, peer).wait()
            return c

        lax.fori_loop(1, n, end, 0)

    def fill_rows(self, place, local):
        picked = dot(place.astype(BF16), local).astype(BF16)
        for s in range(self.groups):
            self.xs[s] = picked[s * self.rows : (s + 1) * self.rows]

    def send_rows(self):
        self.start(lambda p: self.xs.at[p], self.xr, 0)
        self.xr[self.g] = self.xs[self.g]

    def send_partials(self, adapter, store, first_lane, gain=None):
        self.finish(lambda p: self.xs.at[p], self.xr, 0)
        rows = self.xr[...].reshape(self.groups * self.rows, self.xr.shape[2])
        if gain is not None:
            rows = (rows.astype(F32) * gain).astype(BF16)
        total = jnp.zeros((self.groups * self.rows, 128), F32)
        for pair in range(4):
            factors = jnp.concatenate(
                [store[2 * pair, :, 0:128], store[2 * pair + 1, :, 0:128]], axis=1
            )
            both = dot(rows, factors)
            total = total + jnp.where(adapter == 2.0 * pair, both[:, 0:128], 0.0)
            total = total + jnp.where(adapter == 2.0 * pair + 1.0, both[:, 128:256], 0.0)
        half = total.shape[0] // 2
        low, high = total[:half], total[half:]
        if first_lane == 0:
            high = pltpu.roll(high, 64, 1)
        else:
            low = pltpu.roll(low, 64, 1)
        packed = jnp.where(iota(low.shape, 1) < 64, low, high)
        own = half // self.tensors
        for s in range(self.tensors):
            self.ps[s] = packed[s * own : (s + 1) * own]
        self.start(lambda p: self.ps.at[p], self.pr, 1)
        self.pr[self.t] = self.ps[self.t]

    def send_ranks(self):
        self.finish(lambda p: self.ps.at[p], self.pr, 1)
        total = self.pr[0]
        for s in range(1, self.tensors):
            total = total + self.pr[s]
        self.ks[...] = total.astype(BF16)
        self.start(lambda p: self.ks, self.ka, 3)
        self.ka[self.t] = self.ks[...]

    def send_updates(self, adapter, store, first_lane):
        self.finish(lambda p: self.ks, self.ka, 3)
        packed = self.ka[...].astype(F32).reshape(self.groups * self.rows // 2, 128)
        turned = pltpu.roll(packed, 64, 1)
        low, high = (packed, turned) if first_lane == 0 else (turned, packed)
        rank = jnp.concatenate([low, high], axis=0)
        lane = iota(rank.shape, 1)
        rank = jnp.where((lane >= first_lane) & (lane < first_lane + 64), rank, 0.0)
        total = None
        for pair in range(4):
            low = jnp.concatenate(
                [
                    jnp.where(adapter == 2.0 * pair, rank, 0.0),
                    jnp.where(adapter == 2.0 * pair + 1.0, rank, 0.0),
                ],
                axis=1,
            ).astype(BF16)
            factors = jnp.concatenate(
                [store[2 * pair, :, 128:256], store[2 * pair + 1, :, 128:256]], axis=1
            )
            part = dot_nt(low, factors)
            total = part if total is None else total + part
        total = total.astype(BF16)
        for s in range(self.groups):
            self.ds[s] = total[s * self.rows : (s + 1) * self.rows]
        self.start(lambda p: self.ds.at[p], self.dr, 2)
        self.dr[self.g] = self.ds[self.g]

    def update(self, place):
        self.finish(lambda p: self.ds.at[p], self.dr, 2)
        rows = self.dr[...].reshape(self.groups * self.rows, self.dr.shape[2])
        return adapter_scale * dot(place.T.astype(BF16), rows)


def lora_scratch(sizes, cap, width):
    groups, tensors = sizes
    own = groups * cap * SEG // 2 // tensors
    big = max(groups, tensors)
    return [
        pltpu.VMEM((groups, cap * SEG, width), BF16),
        pltpu.VMEM((groups, cap * SEG, width), BF16),
        pltpu.VMEM((tensors, own, 128), F32),
        pltpu.VMEM((tensors, own, 128), F32),
        pltpu.VMEM((own, 128), BF16),
        pltpu.VMEM((tensors, own, 128), BF16),
        pltpu.VMEM((groups, cap * SEG, width), BF16),
        pltpu.VMEM((groups, cap * SEG, width), BF16),
        pltpu.SemaphoreType.DMA((4, big)),
        pltpu.SemaphoreType.DMA((4, big)),
    ]


def owners(order, counts, trims, half, part, own_ref, used_ref):
    rows, pool = counts.shape[1], order.shape[1]
    square = (rows, rows)
    diag = iota(square, 0) == iota(square, 1)
    count_col = jnp.sum(jnp.where(diag, counts, 0.0), axis=1, keepdims=True)
    offsets = jnp.sum(
        jnp.where(iota(square, 0) < iota(square, 1), count_col, 0.0), axis=0, keepdims=True
    )
    lengths = counts * (2 * half) - trims
    spot = jnp.sum(
        jnp.where(
            order == iota((pool, pool), 0).astype(F32), iota((pool, pool), 1).astype(F32), 0.0
        ),
        axis=1,
        keepdims=True,
    )
    owner = (spot >= offsets) & (spot < offsets + counts)
    own_ref[...] = jnp.where(owner, 1.0, 0.0)
    first = (part * half).astype(F32)
    used = jnp.sum(
        jnp.where(owner, lengths - (spot - offsets) * (2 * half) - first, 0.0),
        axis=1,
        keepdims=True,
    )
    used_ref[...] = jnp.broadcast_to(used, (pool, 128))
    return jnp.sum(jnp.where(diag, lengths, 0.0), axis=1, keepdims=True)


def attend(own, side, q, kv_ref, half, work):
    used_ref, qp_ref, op_ref, mp_ref, lp_ref = work
    pool, rows = own.shape
    heads = q.shape[1] // HD
    block = NB // half
    used = used_ref[:, 0:1]
    qp_ref[side] = dot(own.astype(BF16), q)
    wide = (block * heads, NB)
    same_page = (iota(wide, 1) // half) == (iota(wide, 0) & (block - 1))
    slot = (iota(wide, 1) & (half - 1)).astype(F32)
    for b in range(pool // block):
        pages = slice(b * block, (b + 1) * block)
        query = jnp.concatenate(
            [qp_ref[side, pages, h * HD : (h + 1) * HD] for h in range(heads)], axis=0
        ).astype(BF16)
        keys = kv_ref[b * NB : (b + 1) * NB, 0:HD]
        values = kv_ref[b * NB : (b + 1) * NB, HD : 2 * HD]
        scores = dot_nt(query, keys) / math.sqrt(HD)
        limit = jnp.concatenate([used[pages]] * heads, axis=0)
        usable = same_page & (slot < limit)
        masked = jnp.where(usable, scores, far_score)
        top = jnp.max(masked, axis=1, keepdims=True)
        weights = jnp.where(usable, jnp.exp(masked - top), 0.0).astype(BF16)
        total = jnp.sum(weights.astype(F32), axis=1, keepdims=True)
        op_ref[side, b] = dot(weights, values)
        mp_ref[side, b] = jnp.broadcast_to(top, (block * heads, HD))
        lp_ref[side, b] = jnp.broadcast_to(total, (block * heads, HD))


def join_pages(own_ref, own_t, side, half, work, emit):
    used_ref, qp_ref, op_ref, mp_ref, lp_ref = work
    pool, rows = own_ref.shape
    block = NB // half
    heads = op_ref.shape[2] // block
    diag = iota((rows, rows), 0) == iota((rows, rows), 1)
    lane = iota((rows, HD), 1)
    summary = jnp.zeros((rows, HD), F32)
    for h in range(heads):
        inner = slice(h * block, (h + 1) * block)
        top = jnp.full((block, rows), far_score, F32)
        for b in range(pool // block):
            mine = own_ref[b * block : (b + 1) * block, :] > 0.0
            top = jnp.maximum(top, jnp.where(mine, mp_ref[side, b, inner, :], far_score))
        top = jnp.max(top, axis=0, keepdims=True)
        total = jnp.zeros((block, rows), F32)
        scaled = []
        for b in range(pool // block):
            mine = own_ref[b * block : (b + 1) * block, :] > 0.0
            page_top = jnp.max(jnp.where(mine, top, far_score), axis=1, keepdims=True)
            factor = jnp.exp(mp_ref[side, b, inner, :] - page_top)
            scaled.append(op_ref[side, b, inner, :] * factor)
            total = total + jnp.where(mine, lp_ref[side, b, inner, :] * factor, 0.0)
        total = jnp.sum(total, axis=0, keepdims=True)
        emit(h, dot(own_t, jnp.concatenate(scaled, axis=0).astype(BF16)))
        top_col = jnp.sum(jnp.where(diag, top, 0.0), axis=1, keepdims=True)
        total_col = jnp.sum(jnp.where(diag, total, 0.0), axis=1, keepdims=True)
        summary = jnp.where(lane == h, top_col, summary)
        summary = jnp.where(lane == 8 + h, total_col, summary)
    return summary


class Torus:
    def __init__(self, g, t):
        self.g, self.y, self.z = g, t // SIDE, lax.rem(t, SIDE)

    def at(self, h, da, db):
        dy, dz = (da, db) if h == 0 else (db, da)
        return lax.rem(self.y + dy, SIDE) * SIDE + lax.rem(self.z + dz, SIDE)

    def near(self, h, level, sign):
        step = 1 if sign > 0 else SIDE - 1
        return (self.g, self.at(h, step, 0) if level < 4 else self.at(h, 0, step))


def layer_kernel(
    sizes, cap,
    small_ref, gain_raw,
    hidden_hbm, matrix_hbm, store_hbm, kv_hbm, weight_hbm,
    out_ref,
    own_hidden, hidden_ref, matrix_ref, store_ref, kv_ref, weight_ref,
    gain_ref, normed_ref, inv_ref, acc_ref, q_ref,
    own_ref, used_ref, qp_ref, op_ref, mp_ref, lp_ref, o_ref, ml_ref, ms_ref,
    os_ref, or_ref, mr_ref, att_ref, snd, rcv, keep, mine, fin,
    load_sem, chunk_sem, pair_sem, rs_s, rs_r, ag_s, ag_r,
    *lora_refs,
):
    g, t = lax.axis_index("group"), lax.axis_index("tensor")
    all_in = enter(sizes, g, t)
    part = lax.rem(t, 2)
    partner = t + 1 - 2 * part
    chunks, depth, width = matrix_ref.shape
    rows, model = hidden_ref.shape
    pool = own_ref.shape[0]
    half = kv_ref.shape[0] // pool
    own_cols = pl.ds(pl.multiple_of(t * width, width), width)

    order = small_ref[:, 0:pool]
    counts = small_ref[:, 256 : 256 + rows]
    trims = small_ref[:, 384 : 384 + rows]
    segs = sizes[0] * 8
    route = small_ref[:, 512 : 512 + segs]
    slots = small_ref[:, 640 : 640 + segs]
    own_load = pltpu.make_async_copy(hidden_hbm.at[:, own_cols], own_hidden, load_sem.at[4])
    hidden_load, store_load, kv_load, weight_load = [
        pltpu.make_async_copy(src, dst, load_sem.at[i])
        for i, (src, dst) in enumerate(
            (
                (hidden_hbm, hidden_ref), (store_hbm, store_ref), (kv_hbm, kv_ref),
                (weight_hbm, weight_ref),
            )
        )
    ]
    chunk_loads = [
        pltpu.make_async_copy(
            matrix_hbm.at[pl.ds(k * depth, depth), :], matrix_ref.at[k], chunk_sem.at[k]
        )
        for k in range(chunks)
    ]
    own_load.start()
    hidden_load.start()
    chunk_loads[0].start()
    store_load.start()
    for load in chunk_loads[1:]:
        load.start()
    own_load.wait()
    place, adapter = selection(route, slots, g, sizes[0], cap)
    lora_q = Lora(lora_refs[:10], sizes, g, t, cap)
    lora = Lora(lora_refs[10:], sizes, g, t, cap)
    torus = Torus(g, t)
    lora_q.fill_rows(place, own_hidden[...])
    all_in()
    lora_q.send_rows()
    gain = gain_raw[...].astype(F32)
    for k in range(model // 128):
        gain_ref[:, k * 128 : (k + 1) * 128] = gain[k : k + 1, :]

    hidden_load.wait()

    def squares(r, c):
        at = pl.ds(pl.multiple_of(r * 16, 16), 16)
        total = jnp.zeros((16, 128), F32)
        for k in range(model // 1024):
            x = hidden_ref[at, k * 1024 : (k + 1) * 1024].astype(F32)
            x = x * x
            for j in range(8):
                total = total + x[:, j * 128 : (j + 1) * 128]
        mean = jnp.sum(total, axis=1, keepdims=True) / model
        inv = lax.rsqrt(mean + norm_eps)
        inv_ref[at, :] = jnp.broadcast_to(inv, (16, 128))
        for k in range(model // 1024):
            cols = slice(k * 1024, (k + 1) * 1024)
            normed_ref[at, cols] = (
                hidden_ref[at, cols].astype(F32) * inv * gain_ref[:, cols]
            ).astype(BF16)
        return c

    lax.fori_loop(0, rows // 16, squares, 0)

    def project(k):
        chunk_loads[k].wait()
        product = dot(normed_ref[:, k * depth : (k + 1) * depth], matrix_ref[k])
        acc_ref[...] = product if k == 0 else acc_ref[...] + product

    for k in range(chunks - 2):
        project(k)
    kv_load.start()
    weight_load.start()
    store_load.wait()
    lora_q.send_partials(adapter, store_ref, 0, gain_ref[:, own_cols])
    for k in range(chunks - 2, chunks):
        project(k)
    lengths = owners(order, counts, trims, half, part, own_ref, used_ref)
    lora_q.send_ranks()
    spin = iota((1, HD), 1) & (HD // 2 - 1)
    frequency = jnp.exp(spin.astype(F32) * (-2.0 * math.log(rope_base) / HD))
    angles = (lengths - 1.0) * frequency
    cos_table = jnp.cos(angles)
    sin_table = jnp.sin(angles) * jnp.where(iota((1, HD), 1) < HD // 2, -1.0, 1.0)
    lora_q.send_updates(adapter, store_ref, 0)
    full = acc_ref[...] + inv_ref[:, 0:1] * lora_q.update(place)
    heads = []
    for h in range(width // HD):
        x = full[:, h * HD : (h + 1) * HD]
        heads.append(x * cos_table + pltpu.roll(x, HD // 2, 1) * sin_table)
    q_ref[0] = jnp.concatenate(heads, axis=1).astype(BF16)

    def pair_copy(src, dst, i):
        return pltpu.make_async_remote_copy(
            src_ref=src, dst_ref=dst, send_sem=pair_sem.at[0, i], recv_sem=pair_sem.at[1, i],
            device_id=(g, partner), device_id_type=MESH,
        )

    query_copy = pair_copy(q_ref.at[0], q_ref.at[1], 5)
    query_copy.start()
    work = (used_ref, qp_ref, op_ref, mp_ref, lp_ref)
    own = own_ref[...]
    own_t = own.T.astype(BF16)
    kv_load.wait()
    attend(own, 0, q_ref[0], kv_ref, half, work)
    query_copy.wait()
    attend(own, 1, q_ref[1], kv_ref, half, work)
    copies = [
        pair_copy(
            os_ref.at[:, pl.ds(h * HD, HD)], or_ref.at[:, pl.ds(h * HD, HD)], h
        )
        for h in range(width // HD)
    ]

    def give(h, value):
        os_ref[:, h * HD : (h + 1) * HD] = value.astype(BF16)
        copies[h].start()

    def hold(h, value):
        o_ref[:, h * HD : (h + 1) * HD] = value

    ms_ref[...] = join_pages(own_ref, own_t, 1, half, work, give)
    summary_copy = pair_copy(ms_ref, mr_ref, 4)
    summary_copy.start()
    ml_ref[...] = join_pages(own_ref, own_t, 0, half, work, hold)
    summary_copy.wait()
    for h in range(width // HD):
        cols = slice(h * HD, (h + 1) * HD)
        own_top, other_top = ml_ref[:, h : h + 1], mr_ref[:, h : h + 1]
        top = jnp.maximum(own_top, other_top)
        own_scale, other_scale = jnp.exp(own_top - top), jnp.exp(other_top - top)
        total = ml_ref[:, 8 + h : 9 + h] * own_scale + mr_ref[:, 8 + h : 9 + h] * other_scale
        copies[h].wait()
        joined = o_ref[:, cols] * own_scale + or_ref[:, cols].astype(F32) * other_scale
        att_ref[:, cols] = (joined / total).astype(BF16)

    lora.fill_rows(place, att_ref[...])
    lora.send_rows()

    def block(h, da, db):
        col = torus.at(h, da, db) * (2 * NB) + h * NB
        return dot(att_ref[...], weight_ref[:, pl.ds(pl.multiple_of(col, NB), NB)])

    def copy_of(h, level, kind):
        return pltpu.make_async_remote_copy(
            src_ref=snd.at[h, level, kind], dst_ref=rcv.at[h, level, kind],
            send_sem=rs_s.at[h, level, kind], recv_sem=rs_r.at[h, level, kind],
            device_id=torus.near(h, level, 1 if kind % 2 == 0 else -1), device_id_type=MESH,
        )

    def send(h, level, kind, value):
        snd[h, level, kind] = value.astype(BF16)
        copy_of(h, level, kind).start()

    def got(h, level, kind):
        copy_of(h, level, kind).wait_recv()
        return rcv[h, level, kind].astype(F32)

    def send_far(h, level, value):
        send(h, level, 0, value[:64])
        send(h, level, 1, value[64:])

    def send_plus(h, level, value):
        send(h, level, 2, value[64:])
        keep[h, level, 0] = value[:64]

    def send_minus(h, level, value):
        send(h, level, 3, value[:64])
        keep[h, level, 1] = value[64:]

    def relay(h, level):
        send(h, level, 4, keep[h, level, 0] + got(h, level, 0))
        send(h, level, 5, keep[h, level, 1] + got(h, level, 1))

    def arrived(h, level, value):
        upper = value[:64] + got(h, level, 3) + got(h, level, 4)
        lower = value[64:] + got(h, level, 2) + got(h, level, 5)
        return jnp.concatenate([upper, lower], axis=0)

    weight_load.wait()
    for level, db in enumerate(orders):
        for h in range(2):
            send_far(h, level, block(h, 2, db))
    for level, db in enumerate(orders):
        for h in range(2):
            send_plus(h, level, block(h, 1, db))
            send_minus(h, level, block(h, 3, db))
    for level, db in enumerate(orders):
        for h in range(2):
            mine[h, level] = block(h, 0, db)
    lora.send_partials(adapter, store_ref, 64)
    for level in range(4):
        for h in range(2):
            relay(h, level)
    lora.send_ranks()
    for level in range(4):
        for h in range(2):
            value = arrived(h, level, mine[h, level])
            if level == 0:
                send_far(h, 4, value)
            elif level == 1:
                send_plus(h, 4, value)
            elif level == 2:
                send_minus(h, 4, value)
            else:
                fin[h] = value
    lora.send_updates(adapter, store_ref, 64)
    for h in range(2):
        relay(h, 4)
    update = lora.update(place)
    for h in range(2):
        cols = slice(h * NB, (h + 1) * NB)
        total = arrived(h, 4, fin[h]) + update[:, cols] + own_hidden[:, cols].astype(F32)
        col = t * width + h * NB
        out_ref[:, pl.ds(pl.multiple_of(col, NB), NB)] = total.astype(BF16)

    def spread(h, level, kind, da, db):
        col = torus.at(h, da, db) * (2 * NB) + h * NB
        upper = kind in (0, 3, 4)
        half_rows = out_ref.shape[0] // 2
        rows = slice(0, half_rows) if upper else slice(half_rows, 2 * half_rows)
        place_at = out_ref.at[rows, pl.ds(pl.multiple_of(col, NB), NB)]
        return pltpu.make_async_remote_copy(
            src_ref=place_at, dst_ref=place_at,
            send_sem=ag_s.at[h, level, kind], recv_sem=ag_r.at[h, level, kind],
            device_id=torus.near(h, level, 1 if kind % 2 == 0 else -1), device_id_type=MESH,
        )

    sent = (0, 0, 0, 0, 3, 1)
    brought = (3, 1, 3, 1, 2, 2)

    def go(h, level, kind):
        if level == 4:
            spread(h, level, kind, 0, sent[kind]).start()
        else:
            spread(h, level, kind, sent[kind], level).start()

    def came(h, level, kind):
        if level == 4:
            spread(h, level, kind, 0, brought[kind]).wait_recv()
        else:
            spread(h, level, kind, brought[kind], level).wait_recv()

    def left(h, level, kind):
        if level == 4:
            spread(h, level, kind, 0, sent[kind]).wait_send()
        else:
            spread(h, level, kind, sent[kind], level).wait_send()

    def go_all(h, level, kinds):
        for kind in kinds:
            go(h, level, kind)

    def pass_on(h, level):
        came(h, level, 0)
        go(h, level, 4)
        came(h, level, 1)
        go(h, level, 5)

    for level in (4, 0):
        for h in range(2):
            go_all(h, level, range(4))
    for h in range(2):
        pass_on(h, 4)
        go_all(h, 3, (0, 3))
        go_all(h, 1, (1, 2))
    for h in range(2):
        came(h, 4, 2)
        go_all(h, 3, (2, 1))
        came(h, 4, 3)
        go_all(h, 1, (0, 3))
    for h in range(2):
        pass_on(h, 0)
    for h in range(2):
        came(h, 4, 4)
        go_all(h, 2, (0, 3))
        came(h, 4, 5)
        go_all(h, 2, (1, 2))
    for level in (3, 1, 2):
        for h in range(2):
            pass_on(h, level)
    for level in (0, 3, 1, 2):
        for h in range(2):
            for kind in range(2, 6):
                came(h, level, kind)
    for level in range(5):
        for h in range(2):
            for kind in range(6):
                copy_of(h, level, kind).wait_send()
                left(h, level, kind)


def body(
    sizes,
    hidden, norm_gain, query_matrix, output_weight, kv_pages, page_order, page_counts,
    page_trims, adapter_store, store_route, store_slot,
):
    groups = sizes[0]
    cap = max(2, 16 // groups) if groups > 1 else 8
    rows, width = hidden.shape
    local_width = query_matrix.shape[1]
    pool, _, half, lanes = kv_pages.shape
    stored = adapter_store.shape[0]
    hbm = pl.BlockSpec(memory_space=pltpu.HBM)
    vmem = pl.BlockSpec(memory_space=pltpu.VMEM)

    def at_lane(value, first):
        row = value.reshape(1, -1)
        return jnp.pad(row, ((0, 0), (first, 768 - first - row.shape[1])))

    small = (
        at_lane(page_order, 0) + at_lane(page_counts, 256) + at_lane(page_trims, 384)
        + at_lane(store_route, 512) + at_lane(store_slot, 640)
    ).astype(F32)
    chunks = 8
    blocks = pool * half // NB
    block_rows = (NB // half) * (local_width // HD)
    return pl.pallas_call(
        functools.partial(layer_kernel, sizes, cap),
        out_shape=jax.ShapeDtypeStruct((rows, width), BF16),
        in_specs=[vmem] * 2 + [hbm] * 5,
        out_specs=vmem,
        scratch_shapes=[
            pltpu.VMEM((rows, local_width), BF16),
            pltpu.VMEM((rows, width), BF16),
            pltpu.VMEM((chunks, width // chunks, local_width), BF16),
            pltpu.VMEM((stored, local_width, lanes), BF16),
            pltpu.VMEM((pool * half, lanes), BF16),
            pltpu.VMEM((local_width, width), BF16),
            pltpu.VMEM((1, width), F32),
            pltpu.VMEM((rows, width), BF16),
            pltpu.VMEM((rows, 128), F32),
            pltpu.VMEM((rows, local_width), F32),
            pltpu.VMEM((2, rows, local_width), BF16),
            pltpu.VMEM((pool, rows), F32),
            pltpu.VMEM((pool, 128), F32),
            pltpu.VMEM((2, pool, local_width), F32),
            pltpu.VMEM((2, blocks, block_rows, HD), F32),
            pltpu.VMEM((2, blocks, block_rows, HD), F32),
            pltpu.VMEM((2, blocks, block_rows, HD), F32),
            pltpu.VMEM((rows, local_width), F32),
            pltpu.VMEM((rows, 128), F32),
            pltpu.VMEM((rows, 128), F32),
            pltpu.VMEM((rows, local_width), BF16),
            pltpu.VMEM((rows, local_width), BF16),
            pltpu.VMEM((rows, 128), F32),
            pltpu.VMEM((rows, local_width), BF16),
            pltpu.VMEM((2, 5, 6, rows // 2, NB), BF16),
            pltpu.VMEM((2, 5, 6, rows // 2, NB), BF16),
            pltpu.VMEM((2, 5, 2, rows // 2, NB), F32),
            pltpu.VMEM((2, 4, rows, NB), F32),
            pltpu.VMEM((2, rows, NB), F32),
            pltpu.SemaphoreType.DMA((5,)),
            pltpu.SemaphoreType.DMA((chunks,)),
            pltpu.SemaphoreType.DMA((2, 6)),
            pltpu.SemaphoreType.DMA((2, 5, 6)),
            pltpu.SemaphoreType.DMA((2, 5, 6)),
            pltpu.SemaphoreType.DMA((2, 5, 6)),
            pltpu.SemaphoreType.DMA((2, 5, 6)),
        ]
        + lora_scratch(sizes, cap, local_width)
        + lora_scratch(sizes, cap, local_width),
        compiler_params=pltpu.CompilerParams(
            collective_id=0, has_side_effects=True, vmem_limit_bytes=50 << 20
        ),
        name="layer",
    )(
        small, norm_gain.reshape(width // 128, 128), hidden, query_matrix, adapter_store, kv_pages.reshape(pool * half, lanes), output_weight,
    )


def solution(mesh):
    sizes = (mesh.shape["group"], mesh.shape["tensor"])
    in_specs = (
        P("group", None),
        P(),
        P(None, "tensor"),
        P("tensor", None),
        P("group", "tensor", None, None),
        P("group", None),
        P("group", None),
        P("group", None),
        P("group", "tensor", None),
        P(),
        P(),
    )
    return jax.shard_map(
        functools.partial(body, sizes),
        mesh=mesh,
        in_specs=in_specs,
        out_specs=P("group", None),
        check_vma=False,
    )
```

```python
import functools
import math

import jax
import jax.numpy as jnp
from jax import lax
from jax.experimental import pallas as pl
from jax.experimental.pallas import tpu as pltpu
from jax.sharding import PartitionSpec as P

MESH = pl.DeviceIdType.MESH
F32 = jnp.float32
BF16 = jnp.bfloat16

KVH = 8
HD = 128
SEG = 16
SIDE = 4
NB = 256
adapter_scale = 2.0
norm_eps = 1e-05
rope_base = 500000.0
far_score = -1e30
orders = (2, 1, 3, 0)


def iota(shape, dim):
    return lax.broadcasted_iota(jnp.int32, shape, dim)


def dot(a, b):
    return jnp.dot(a, b, preferred_element_type=F32)


def dot_nt(a, b):
    return lax.dot_general(a, b, (((1,), (1,)), ((), ())), preferred_element_type=F32)


def enter(sizes, g, t):
    groups, tensors = sizes
    barrier = pltpu.get_barrier_semaphore()

    def greet_tensor(d, c):
        pl.semaphore_signal(
            barrier, inc=1, device_id=(g, lax.rem(t + d, tensors)), device_id_type=MESH
        )
        return c

    def greet_group(d, c):
        pl.semaphore_signal(
            barrier, inc=1, device_id=(lax.rem(g + d, groups), t), device_id_type=MESH
        )
        return c

    lax.fori_loop(1, tensors, greet_tensor, 0)
    lax.fori_loop(1, groups, greet_group, 0)
    return lambda: pl.semaphore_wait(barrier, groups + tensors - 2)


def selection(route_row, slots, g, groups, cap):
    slot_rows = groups * cap * SEG
    segs = groups * 8
    value_row = slots + 1.0
    lane, sub = iota((segs, segs), 1), iota((segs, segs), 0)
    diag = lane == sub
    route_col = jnp.sum(jnp.where(diag, route_row, 0.0), axis=1, keepdims=True)
    me = g.astype(F32)
    mine = jnp.where(route_col == me, 1.0, 0.0)
    mine_row = jnp.where(route_row == me, 1.0, 0.0)
    rank = jnp.sum(
        jnp.where(((lane >> 3) == (sub >> 3)) & (lane < sub), mine_row, 0.0),
        axis=1,
        keepdims=True,
    )
    spot = mine * ((iota((segs, 1), 0) >> 3).astype(F32) * cap + rank + 1.0)
    spot_row = jnp.sum(jnp.where(diag, spot, 0.0), axis=0, keepdims=True)
    row_slot = (iota((slot_rows, segs), 0) >> 4).astype(F32) + 1.0
    adapter = jnp.sum(jnp.where(spot_row == row_slot, value_row, 0.0), axis=1, keepdims=True) - 1.0
    lane, sub = iota((segs, 128), 1), iota((segs, 128), 0)
    own_seg = lane >> 4
    in_group = (sub >> 3) == g
    r_row = jnp.sum(
        jnp.where(in_group & (own_seg == (sub & 7)), route_col, 0.0), axis=0, keepdims=True
    )
    rank = jnp.sum(
        jnp.where(in_group & (route_col == r_row) & ((sub & 7) < own_seg), 1.0, 0.0),
        axis=0,
        keepdims=True,
    )
    in_seg = (iota((1, 128), 1) & 15).astype(F32)
    spot = (r_row * cap + rank) * SEG + in_seg
    place = jnp.where(iota((slot_rows, 128), 0).astype(F32) == spot, 1.0, 0.0)
    return place, adapter


class Lora:
    def __init__(self, refs, sizes, g, t, cap):
        (
            self.xs, self.xr, self.ps, self.pr, self.ks, self.ka, self.ds, self.dr,
            self.ssem, self.rsem,
        ) = refs
        self.groups, self.tensors = sizes
        self.g, self.t, self.cap = g, t, cap
        self.rows = cap * SEG

    def pair_copy(self, src, dst, stage, peer, at):
        return pltpu.make_async_remote_copy(
            src_ref=src, dst_ref=dst,
            send_sem=self.ssem.at[stage, peer], recv_sem=self.rsem.at[stage, at],
            device_id=(peer, self.t) if stage % 2 == 0 else (self.g, peer),
            device_id_type=MESH,
        )

    def start(self, src_of, dst, stage):
        me, n = (self.g, self.groups) if stage % 2 == 0 else (self.t, self.tensors)

        def send(d, c):
            peer = lax.rem(me + d, n)
            self.pair_copy(src_of(peer), dst.at[me], stage, peer, me).start()
            return c

        lax.fori_loop(1, n, send, 0)

    def finish(self, src_of, dst, stage):
        me, n = (self.g, self.groups) if stage % 2 == 0 else (self.t, self.tensors)

        def end(d, c):
            peer = lax.rem(me + d, n)
            self.pair_copy(src_of(peer), dst.at[peer], stage, peer, peer).wait()
            return c

        lax.fori_loop(1, n, end, 0)

    def fill_rows(self, place, local):
        picked = dot(place.astype(BF16), local).astype(BF16)
        for s in range(self.groups):
            self.xs[s] = picked[s * self.rows : (s + 1) * self.rows]

    def send_rows(self):
        self.start(lambda p: self.xs.at[p], self.xr, 0)
        self.xr[self.g] = self.xs[self.g]

    def send_partials(self, adapter, store, first_lane, gain=None):
        self.finish(lambda p: self.xs.at[p], self.xr, 0)
        rows = self.xr[...].reshape(self.groups * self.rows, self.xr.shape[2])
        if gain is not None:
            rows = (rows.astype(F32) * gain).astype(BF16)
        total = jnp.zeros((self.groups * self.rows, 128), F32)
        for pair in range(4):
            factors = jnp.concatenate(
                [store[2 * pair, :, 0:128], store[2 * pair + 1, :, 0:128]], axis=1
            )
            both = dot(rows, factors)
            total = total + jnp.where(adapter == 2.0 * pair, both[:, 0:128], 0.0)
            total = total + jnp.where(adapter == 2.0 * pair + 1.0, both[:, 128:256], 0.0)
        half = total.shape[0] // 2
        low, high = total[:half], total[half:]
        if first_lane == 0:
            high = pltpu.roll(high, 64, 1)
        else:
            low = pltpu.roll(low, 64, 1)
        packed = jnp.where(iota(low.shape, 1) < 64, low, high)
        own = half // self.tensors
        for s in range(self.tensors):
            self.ps[s] = packed[s * own : (s + 1) * own]
        self.start(lambda p: self.ps.at[p], self.pr, 1)
        self.pr[self.t] = self.ps[self.t]

    def send_ranks(self):
        self.finish(lambda p: self.ps.at[p], self.pr, 1)
        total = self.pr[0]
        for s in range(1, self.tensors):
            total = total + self.pr[s]
        self.ks[...] = total.astype(BF16)
        self.start(lambda p: self.ks, self.ka, 3)
        self.ka[self.t] = self.ks[...]

    def send_updates(self, adapter, store, first_lane):
        self.finish(lambda p: self.ks, self.ka, 3)
        packed = self.ka[...].astype(F32).reshape(self.groups * self.rows // 2, 128)
        turned = pltpu.roll(packed, 64, 1)
        low, high = (packed, turned) if first_lane == 0 else (turned, packed)
        rank = jnp.concatenate([low, high], axis=0)
        lane = iota(rank.shape, 1)
        rank = jnp.where((lane >= first_lane) & (lane < first_lane + 64), rank, 0.0)
        total = None
        for pair in range(4):
            low = jnp.concatenate(
                [
                    jnp.where(adapter == 2.0 * pair, rank, 0.0),
                    jnp.where(adapter == 2.0 * pair + 1.0, rank, 0.0),
                ],
                axis=1,
            ).astype(BF16)
            factors = jnp.concatenate(
                [store[2 * pair, :, 128:256], store[2 * pair + 1, :, 128:256]], axis=1
            )
            part = dot_nt(low, factors)
            total = part if total is None else total + part
        total = total.astype(BF16)
        for s in range(self.groups):
            self.ds[s] = total[s * self.rows : (s + 1) * self.rows]
        self.start(lambda p: self.ds.at[p], self.dr, 2)
        self.dr[self.g] = self.ds[self.g]

    def update(self, place):
        self.finish(lambda p: self.ds.at[p], self.dr, 2)
        rows = self.dr[...].reshape(self.groups * self.rows, self.dr.shape[2])
        return adapter_scale * dot(place.T.astype(BF16), rows)


    def send_group_partials(self, rows, spot, factors):
        lane_half = iota((rows.shape[0], 128), 1) >> 6
        total = jnp.zeros((rows.shape[0], 128), F32)
        for pair in range(self.groups // 2):
            both = dot(rows, jnp.concatenate([factors[2 * pair], factors[2 * pair + 1]], axis=1))
            for i in range(2):
                mine = (spot - 2 * (2 * pair + i)) == lane_half
                total = total + jnp.where(mine, both[:, i * 128 : (i + 1) * 128], 0.0)
        own = total.shape[0] // self.tensors
        for s in range(self.tensors):
            self.ps[s] = total[s * own : (s + 1) * own]
        self.start(lambda p: self.ps.at[p], self.pr, 1)
        self.pr[self.t] = self.ps[self.t]

    def group_update(self, spot, factors):
        rank = self.ka[...].astype(F32).reshape(-1, 128)
        store = spot >> 1
        total = None
        for pair in range(self.groups // 2):
            low = jnp.concatenate(
                [jnp.where(store == 2 * pair + i, rank, 0.0) for i in range(2)], axis=1
            ).astype(BF16)
            up = jnp.concatenate([factors[2 * pair], factors[2 * pair + 1]], axis=1)
            part = dot_nt(low, up)
            total = part if total is None else total + part
        return adapter_scale * total


class Factors:
    def __init__(self, sems, g, t, groups):
        self.ssem, self.rsem = sems
        self.g, self.t, self.groups = g, t, groups

    def double(self, store, first, twice):
        row, col = iota((128, 128), 0), iota((128, 128), 1)
        repeat = jnp.where(row == 64 + (col & 63), 1.0, 0.0).astype(BF16)
        for a in range(store.shape[0]):
            twice[a] = dot(store[a, :, first : first + 128], repeat).astype(BF16)

    def choose(self, twice, adapter, out, held):
        lane = iota((1, 128), 1)
        for s in range(self.groups):
            left_one = adapter[2 * s * SEG : 2 * s * SEG + 1, :]
            right_one = adapter[(2 * s + 1) * SEG : (2 * s + 1) * SEG + 1, :]
            named = jnp.where(lane < 64, left_one, right_one)
            total = None
            for a in range(twice.shape[0]):
                part = twice[a] * jnp.where(named == 1.0 * a, 1.0, 0.0).astype(BF16)
                total = part if total is None else total + part
            out[s] = total
        held[self.g] = out[self.g]

    def copy(self, out, held, kind, rows, peer, at):
        return pltpu.make_async_remote_copy(
            src_ref=out.at[peer, rows], dst_ref=held.at[at, rows],
            send_sem=self.ssem.at[kind, peer], recv_sem=self.rsem.at[kind, at],
            device_id=(peer, self.t), device_id_type=MESH,
        )

    def start(self, out, held, kind, rows):
        def send(d, c):
            peer = lax.rem(self.g + d, self.groups)
            self.copy(out, held, kind, rows, peer, self.g).start()
            return c

        lax.fori_loop(1, self.groups, send, 0)

    def finish(self, out, held, kind, rows):
        def end(d, c):
            peer = lax.rem(self.g + d, self.groups)
            self.copy(out, held, kind, rows, peer, peer).wait()
            return c

        lax.fori_loop(1, self.groups, end, 0)


def lora_scratch(sizes, cap, width):
    groups, tensors = sizes
    own = groups * cap * SEG // 2 // tensors
    big = max(groups, tensors)
    return [
        pltpu.VMEM((groups, cap * SEG, width), BF16),
        pltpu.VMEM((groups, cap * SEG, width), BF16),
        pltpu.VMEM((tensors, own, 128), F32),
        pltpu.VMEM((tensors, own, 128), F32),
        pltpu.VMEM((own, 128), BF16),
        pltpu.VMEM((tensors, own, 128), BF16),
        pltpu.VMEM((groups, cap * SEG, width), BF16),
        pltpu.VMEM((groups, cap * SEG, width), BF16),
        pltpu.SemaphoreType.DMA((4, big)),
        pltpu.SemaphoreType.DMA((4, big)),
    ]


def owners(order, counts, trims, half, part, own_ref, used_ref):
    rows, pool = counts.shape[1], order.shape[1]
    square = (rows, rows)
    diag = iota(square, 0) == iota(square, 1)
    count_col = jnp.sum(jnp.where(diag, counts, 0.0), axis=1, keepdims=True)
    offsets = jnp.sum(
        jnp.where(iota(square, 0) < iota(square, 1), count_col, 0.0), axis=0, keepdims=True
    )
    lengths = counts * (2 * half) - trims
    spot = jnp.sum(
        jnp.where(
            order == iota((pool, pool), 0).astype(F32), iota((pool, pool), 1).astype(F32), 0.0
        ),
        axis=1,
        keepdims=True,
    )
    owner = (spot >= offsets) & (spot < offsets + counts)
    own_ref[...] = jnp.where(owner, 1.0, 0.0)
    first = (part * half).astype(F32)
    used = jnp.sum(
        jnp.where(owner, lengths - (spot - offsets) * (2 * half) - first, 0.0),
        axis=1,
        keepdims=True,
    )
    used_ref[...] = jnp.broadcast_to(used, (pool, 128))
    return jnp.sum(jnp.where(diag, lengths, 0.0), axis=1, keepdims=True)


def attend(own, side, q, kv_ref, half, work):
    used_ref, qp_ref, op_ref, mp_ref, lp_ref = work
    pool, rows = own.shape
    heads = q.shape[1] // HD
    block = NB // half
    used = used_ref[:, 0:1]
    qp_ref[side] = dot(own.astype(BF16), q)
    wide = (block * heads, NB)
    same_page = (iota(wide, 1) // half) == (iota(wide, 0) & (block - 1))
    slot = (iota(wide, 1) & (half - 1)).astype(F32)
    for b in range(pool // block):
        pages = slice(b * block, (b + 1) * block)
        query = jnp.concatenate(
            [qp_ref[side, pages, h * HD : (h + 1) * HD] for h in range(heads)], axis=0
        ).astype(BF16)
        keys = kv_ref[b * NB : (b + 1) * NB, 0:HD]
        values = kv_ref[b * NB : (b + 1) * NB, HD : 2 * HD]
        scores = dot_nt(query, keys) / math.sqrt(HD)
        limit = jnp.concatenate([used[pages]] * heads, axis=0)
        usable = same_page & (slot < limit)
        masked = jnp.where(usable, scores, far_score)
        top = jnp.max(masked, axis=1, keepdims=True)
        weights = jnp.where(usable, jnp.exp(masked - top), 0.0).astype(BF16)
        total = jnp.sum(weights.astype(F32), axis=1, keepdims=True)
        op_ref[side, b] = dot(weights, values)
        mp_ref[side, b] = jnp.broadcast_to(top, (block * heads, HD))
        lp_ref[side, b] = jnp.broadcast_to(total, (block * heads, HD))


def join_pages(own_ref, own_t, side, half, work, emit):
    used_ref, qp_ref, op_ref, mp_ref, lp_ref = work
    pool, rows = own_ref.shape
    block = NB // half
    heads = op_ref.shape[2] // block
    diag = iota((rows, rows), 0) == iota((rows, rows), 1)
    lane = iota((rows, HD), 1)
    summary = jnp.zeros((rows, HD), F32)
    for h in range(heads):
        inner = slice(h * block, (h + 1) * block)
        top = jnp.full((block, rows), far_score, F32)
        for b in range(pool // block):
            mine = own_ref[b * block : (b + 1) * block, :] > 0.0
            top = jnp.maximum(top, jnp.where(mine, mp_ref[side, b, inner, :], far_score))
        top = jnp.max(top, axis=0, keepdims=True)
        total = jnp.zeros((block, rows), F32)
        scaled = []
        for b in range(pool // block):
            mine = own_ref[b * block : (b + 1) * block, :] > 0.0
            page_top = jnp.max(jnp.where(mine, top, far_score), axis=1, keepdims=True)
            factor = jnp.exp(mp_ref[side, b, inner, :] - page_top)
            scaled.append(op_ref[side, b, inner, :] * factor)
            total = total + jnp.where(mine, lp_ref[side, b, inner, :] * factor, 0.0)
        total = jnp.sum(total, axis=0, keepdims=True)
        emit(h, dot(own_t, jnp.concatenate(scaled, axis=0).astype(BF16)))
        top_col = jnp.sum(jnp.where(diag, top, 0.0), axis=1, keepdims=True)
        total_col = jnp.sum(jnp.where(diag, total, 0.0), axis=1, keepdims=True)
        summary = jnp.where(lane == h, top_col, summary)
        summary = jnp.where(lane == 8 + h, total_col, summary)
    return summary


class Torus:
    def __init__(self, g, t):
        self.g, self.y, self.z = g, t // SIDE, lax.rem(t, SIDE)

    def at(self, h, da, db):
        dy, dz = (da, db) if h == 0 else (db, da)
        return lax.rem(self.y + dy, SIDE) * SIDE + lax.rem(self.z + dz, SIDE)

    def near(self, h, level, sign):
        step = 1 if sign > 0 else SIDE - 1
        return (self.g, self.at(h, step, 0) if level < 4 else self.at(h, 0, step))


def layer_kernel(
    sizes, cap,
    small_ref, gain_raw,
    hidden_hbm, matrix_hbm, store_hbm, kv_hbm, weight_hbm,
    out_ref,
    own_hidden, hidden_ref, matrix_ref, store_ref, kv_ref, weight_ref,
    gain_ref, normed_ref, inv_ref, acc_ref, q_ref,
    own_ref, used_ref, qp_ref, op_ref, mp_ref, lp_ref, o_ref, ml_ref, ms_ref,
    os_ref, or_ref, mr_ref, att_ref, snd, rcv, keep, mine, fin,
    load_sem, chunk_sem, pair_sem, twice, down_s, down_r, up_s, up_r, fac_s, fac_r, rs_s, rs_r, ag_s, ag_r,
    *lora_refs,
):
    g, t = lax.axis_index("group"), lax.axis_index("tensor")
    all_in = enter(sizes, g, t)
    part = lax.rem(t, 2)
    partner = t + 1 - 2 * part
    chunks, depth, width = matrix_ref.shape
    rows, model = hidden_ref.shape
    pool = own_ref.shape[0]
    half = kv_ref.shape[0] // pool
    own_cols = pl.ds(pl.multiple_of(t * width, width), width)

    order = small_ref[:, 0:pool]
    counts = small_ref[:, 256 : 256 + rows]
    trims = small_ref[:, 384 : 384 + rows]
    segs = sizes[0] * 8
    route = small_ref[:, 512 : 512 + segs]
    slots = small_ref[:, 640 : 640 + segs]
    own_load = pltpu.make_async_copy(hidden_hbm.at[:, own_cols], own_hidden, load_sem.at[4])
    hidden_load, store_load, kv_load, weight_load = [
        pltpu.make_async_copy(src, dst, load_sem.at[i])
        for i, (src, dst) in enumerate(
            (
                (hidden_hbm, hidden_ref), (store_hbm, store_ref), (kv_hbm, kv_ref),
                (weight_hbm, weight_ref),
            )
        )
    ]
    chunk_loads = [
        pltpu.make_async_copy(
            matrix_hbm.at[pl.ds(k * depth, depth), :], matrix_ref.at[k], chunk_sem.at[k]
        )
        for k in range(chunks)
    ]
    own_load.start()
    hidden_load.start()
    chunk_loads[0].start()
    store_load.start()
    for load in chunk_loads[1:]:
        load.start()
    own_load.wait()
    place, adapter = selection(route, slots, g, sizes[0], cap)
    lora_q = Lora(lora_refs[:10], sizes, g, t, cap)
    lora = Lora((None, None, *lora_refs[10:14], None, None, *lora_refs[14:]), sizes, g, t, cap)
    factors = Factors((fac_s, fac_r), g, t, sizes[0])
    first_rows, last_rows, all_rows = pl.ds(0, 192), pl.ds(192, width - 192), pl.ds(0, width)
    place_t = place.T
    spot = jnp.sum(
        jnp.where(place_t > 0.0, (iota(place_t.shape, 1) >> 4).astype(F32), 0.0), axis=1, keepdims=True
    ).astype(jnp.int32)
    torus = Torus(g, t)
    lora_q.fill_rows(place, own_hidden[...])
    all_in()
    lora_q.send_rows()
    gain = gain_raw[...].astype(F32)
    for k in range(model // 128):
        gain_ref[:, k * 128 : (k + 1) * 128] = gain[k : k + 1, :]

    hidden_load.wait()

    def squares(r, c):
        at = pl.ds(pl.multiple_of(r * 16, 16), 16)
        total = jnp.zeros((16, 128), F32)
        for k in range(model // 1024):
            x = hidden_ref[at, k * 1024 : (k + 1) * 1024].astype(F32)
            x = x * x
            for j in range(8):
                total = total + x[:, j * 128 : (j + 1) * 128]
        mean = jnp.sum(total, axis=1, keepdims=True) / model
        inv = lax.rsqrt(mean + norm_eps)
        inv_ref[at, :] = jnp.broadcast_to(inv, (16, 128))
        for k in range(model // 1024):
            cols = slice(k * 1024, (k + 1) * 1024)
            normed_ref[at, cols] = (
                hidden_ref[at, cols].astype(F32) * inv * gain_ref[:, cols]
            ).astype(BF16)
        return c

    lax.fori_loop(0, rows // 16, squares, 0)

    def project(k):
        chunk_loads[k].wait()
        product = dot(normed_ref[:, k * depth : (k + 1) * depth], matrix_ref[k])
        acc_ref[...] = product if k == 0 else acc_ref[...] + product

    for k in range(chunks - 2):
        project(k)
    kv_load.start()
    weight_load.start()
    store_load.wait()
    factors.double(store_ref, 0, twice)
    lora_q.send_partials(adapter, store_ref, 0, gain_ref[:, own_cols])
    factors.choose(twice, adapter, down_s, down_r)
    factors.start(down_s, down_r, 0, first_rows)
    for k in range(chunks - 2, chunks):
        project(k)
    lengths = owners(order, counts, trims, half, part, own_ref, used_ref)
    lora_q.send_ranks()
    spin = iota((1, HD), 1) & (HD // 2 - 1)
    frequency = jnp.exp(spin.astype(F32) * (-2.0 * math.log(rope_base) / HD))
    angles = (lengths - 1.0) * frequency
    cos_table = jnp.cos(angles)
    sin_table = jnp.sin(angles) * jnp.where(iota((1, HD), 1) < HD // 2, -1.0, 1.0)
    lora_q.send_updates(adapter, store_ref, 0)
    factors.start(down_s, down_r, 1, last_rows)
    factors.double(store_ref, 128, twice)
    factors.choose(twice, adapter, up_s, up_r)
    factors.start(up_s, up_r, 2, all_rows)
    full = acc_ref[...] + inv_ref[:, 0:1] * lora_q.update(place)
    heads = []
    for h in range(width // HD):
        x = full[:, h * HD : (h + 1) * HD]
        heads.append(x * cos_table + pltpu.roll(x, HD // 2, 1) * sin_table)
    q_ref[0] = jnp.concatenate(heads, axis=1).astype(BF16)

    def pair_copy(src, dst, i):
        return pltpu.make_async_remote_copy(
            src_ref=src, dst_ref=dst, send_sem=pair_sem.at[0, i], recv_sem=pair_sem.at[1, i],
            device_id=(g, partner), device_id_type=MESH,
        )

    query_copy = pair_copy(q_ref.at[0], q_ref.at[1], 5)
    query_copy.start()
    work = (used_ref, qp_ref, op_ref, mp_ref, lp_ref)
    own = own_ref[...]
    own_t = own.T.astype(BF16)
    kv_load.wait()
    attend(own, 0, q_ref[0], kv_ref, half, work)
    query_copy.wait()
    attend(own, 1, q_ref[1], kv_ref, half, work)
    copies = [
        pair_copy(
            os_ref.at[:, pl.ds(h * HD, HD)], or_ref.at[:, pl.ds(h * HD, HD)], h
        )
        for h in range(width // HD)
    ]

    def give(h, value):
        os_ref[:, h * HD : (h + 1) * HD] = value.astype(BF16)
        copies[h].start()

    def hold(h, value):
        o_ref[:, h * HD : (h + 1) * HD] = value

    ms_ref[...] = join_pages(own_ref, own_t, 1, half, work, give)
    summary_copy = pair_copy(ms_ref, mr_ref, 4)
    summary_copy.start()
    ml_ref[...] = join_pages(own_ref, own_t, 0, half, work, hold)
    summary_copy.wait()
    for h in range(width // HD):
        cols = slice(h * HD, (h + 1) * HD)
        own_top, other_top = ml_ref[:, h : h + 1], mr_ref[:, h : h + 1]
        top = jnp.maximum(own_top, other_top)
        own_scale, other_scale = jnp.exp(own_top - top), jnp.exp(other_top - top)
        total = ml_ref[:, 8 + h : 9 + h] * own_scale + mr_ref[:, 8 + h : 9 + h] * other_scale
        copies[h].wait()
        joined = o_ref[:, cols] * own_scale + or_ref[:, cols].astype(F32) * other_scale
        att_ref[:, cols] = (joined / total).astype(BF16)


    def block(h, da, db):
        col = torus.at(h, da, db) * (2 * NB) + h * NB
        return dot(att_ref[...], weight_ref[:, pl.ds(pl.multiple_of(col, NB), NB)])

    def copy_of(h, level, kind):
        return pltpu.make_async_remote_copy(
            src_ref=snd.at[h, level, kind], dst_ref=rcv.at[h, level, kind],
            send_sem=rs_s.at[h, level, kind], recv_sem=rs_r.at[h, level, kind],
            device_id=torus.near(h, level, 1 if kind % 2 == 0 else -1), device_id_type=MESH,
        )

    def send(h, level, kind, value):
        snd[h, level, kind] = value.astype(BF16)
        copy_of(h, level, kind).start()

    def got(h, level, kind):
        copy_of(h, level, kind).wait_recv()
        return rcv[h, level, kind].astype(F32)

    def send_far(h, level, value):
        send(h, level, 0, value[:64])
        send(h, level, 1, value[64:])

    def send_plus(h, level, value):
        send(h, level, 2, value[64:])
        keep[h, level, 0] = value[:64]

    def send_minus(h, level, value):
        send(h, level, 3, value[:64])
        keep[h, level, 1] = value[64:]

    def relay(h, level):
        send(h, level, 4, keep[h, level, 0] + got(h, level, 0))
        send(h, level, 5, keep[h, level, 1] + got(h, level, 1))

    def arrived(h, level, value):
        upper = value[:64] + got(h, level, 3) + got(h, level, 4)
        lower = value[64:] + got(h, level, 2) + got(h, level, 5)
        return jnp.concatenate([upper, lower], axis=0)

    weight_load.wait()
    for level, db in enumerate(orders):
        for h in range(2):
            send_far(h, level, block(h, 2, db))
    factors.finish(down_s, down_r, 0, first_rows)
    factors.finish(down_s, down_r, 1, last_rows)
    lora.send_group_partials(att_ref[...], spot, down_r)
    for level, db in enumerate(orders):
        for h in range(2):
            send_plus(h, level, block(h, 1, db))
            send_minus(h, level, block(h, 3, db))
    for level, db in enumerate(orders):
        for h in range(2):
            mine[h, level] = block(h, 0, db)
    for level in range(4):
        for h in range(2):
            relay(h, level)
    lora.send_ranks()
    for level in range(4):
        for h in range(2):
            value = arrived(h, level, mine[h, level])
            if level == 0:
                send_far(h, 4, value)
            elif level == 1:
                send_plus(h, 4, value)
            elif level == 2:
                send_minus(h, 4, value)
            else:
                fin[h] = value
    for h in range(2):
        relay(h, 4)
    lora.finish(lambda p: lora.ks, lora.ka, 3)
    factors.finish(up_s, up_r, 2, all_rows)
    update = lora.group_update(spot, up_r)
    for h in range(2):
        cols = slice(h * NB, (h + 1) * NB)
        total = arrived(h, 4, fin[h]) + update[:, cols] + own_hidden[:, cols].astype(F32)
        col = t * width + h * NB
        out_ref[:, pl.ds(pl.multiple_of(col, NB), NB)] = total.astype(BF16)

    def spread(h, level, kind, da, db):
        col = torus.at(h, da, db) * (2 * NB) + h * NB
        upper = kind in (0, 3, 4)
        half_rows = out_ref.shape[0] // 2
        rows = slice(0, half_rows) if upper else slice(half_rows, 2 * half_rows)
        place_at = out_ref.at[rows, pl.ds(pl.multiple_of(col, NB), NB)]
        return pltpu.make_async_remote_copy(
            src_ref=place_at, dst_ref=place_at,
            send_sem=ag_s.at[h, level, kind], recv_sem=ag_r.at[h, level, kind],
            device_id=torus.near(h, level, 1 if kind % 2 == 0 else -1), device_id_type=MESH,
        )

    sent = (0, 0, 0, 0, 3, 1)
    brought = (3, 1, 3, 1, 2, 2)

    def go(h, level, kind):
        if level == 4:
            spread(h, level, kind, 0, sent[kind]).start()
        else:
            spread(h, level, kind, sent[kind], level).start()

    def came(h, level, kind):
        if level == 4:
            spread(h, level, kind, 0, brought[kind]).wait_recv()
        else:
            spread(h, level, kind, brought[kind], level).wait_recv()

    def left(h, level, kind):
        if level == 4:
            spread(h, level, kind, 0, sent[kind]).wait_send()
        else:
            spread(h, level, kind, sent[kind], level).wait_send()

    def go_all(h, level, kinds):
        for kind in kinds:
            go(h, level, kind)

    def pass_on(h, level):
        came(h, level, 0)
        go(h, level, 4)
        came(h, level, 1)
        go(h, level, 5)

    for level in (4, 0):
        for h in range(2):
            go_all(h, level, range(4))
    for h in range(2):
        pass_on(h, 4)
        go_all(h, 3, (0, 3))
        go_all(h, 1, (1, 2))
    for h in range(2):
        came(h, 4, 2)
        go_all(h, 3, (2, 1))
        came(h, 4, 3)
        go_all(h, 1, (0, 3))
    for h in range(2):
        pass_on(h, 0)
    for h in range(2):
        came(h, 4, 4)
        go_all(h, 2, (0, 3))
        came(h, 4, 5)
        go_all(h, 2, (1, 2))
    for level in (3, 1, 2):
        for h in range(2):
            pass_on(h, level)
    for level in (0, 3, 1, 2):
        for h in range(2):
            for kind in range(2, 6):
                came(h, level, kind)
    for level in range(5):
        for h in range(2):
            for kind in range(6):
                copy_of(h, level, kind).wait_send()
                left(h, level, kind)


def body(
    sizes,
    hidden, norm_gain, query_matrix, output_weight, kv_pages, page_order, page_counts,
    page_trims, adapter_store, store_route, store_slot,
):
    groups = sizes[0]
    cap = max(2, 16 // groups) if groups > 1 else 8
    rows, width = hidden.shape
    local_width = query_matrix.shape[1]
    pool, _, half, lanes = kv_pages.shape
    stored = adapter_store.shape[0]
    hbm = pl.BlockSpec(memory_space=pltpu.HBM)
    vmem = pl.BlockSpec(memory_space=pltpu.VMEM)

    def at_lane(value, first):
        row = value.reshape(1, -1)
        return jnp.pad(row, ((0, 0), (first, 768 - first - row.shape[1])))

    small = (
        at_lane(page_order, 0) + at_lane(page_counts, 256) + at_lane(page_trims, 384)
        + at_lane(store_route, 512) + at_lane(store_slot, 640)
    ).astype(F32)
    chunks = 8
    blocks = pool * half // NB
    block_rows = (NB // half) * (local_width // HD)
    return pl.pallas_call(
        functools.partial(layer_kernel, sizes, cap),
        out_shape=jax.ShapeDtypeStruct((rows, width), BF16),
        in_specs=[vmem] * 2 + [hbm] * 5,
        out_specs=vmem,
        scratch_shapes=[
            pltpu.VMEM((rows, local_width), BF16),
            pltpu.VMEM((rows, width), BF16),
            pltpu.VMEM((chunks, width // chunks, local_width), BF16),
            pltpu.VMEM((stored, local_width, lanes), BF16),
            pltpu.VMEM((pool * half, lanes), BF16),
            pltpu.VMEM((local_width, width), BF16),
            pltpu.VMEM((1, width), F32),
            pltpu.VMEM((rows, width), BF16),
            pltpu.VMEM((rows, 128), F32),
            pltpu.VMEM((rows, local_width), F32),
            pltpu.VMEM((2, rows, local_width), BF16),
            pltpu.VMEM((pool, rows), F32),
            pltpu.VMEM((pool, 128), F32),
            pltpu.VMEM((2, pool, local_width), F32),
            pltpu.VMEM((2, blocks, block_rows, HD), F32),
            pltpu.VMEM((2, blocks, block_rows, HD), F32),
            pltpu.VMEM((2, blocks, block_rows, HD), F32),
            pltpu.VMEM((rows, local_width), F32),
            pltpu.VMEM((rows, 128), F32),
            pltpu.VMEM((rows, 128), F32),
            pltpu.VMEM((rows, local_width), BF16),
            pltpu.VMEM((rows, local_width), BF16),
            pltpu.VMEM((rows, 128), F32),
            pltpu.VMEM((rows, local_width), BF16),
            pltpu.VMEM((2, 5, 6, rows // 2, NB), BF16),
            pltpu.VMEM((2, 5, 6, rows // 2, NB), BF16),
            pltpu.VMEM((2, 5, 2, rows // 2, NB), F32),
            pltpu.VMEM((2, 4, rows, NB), F32),
            pltpu.VMEM((2, rows, NB), F32),
            pltpu.SemaphoreType.DMA((5,)),
            pltpu.SemaphoreType.DMA((chunks,)),
            pltpu.SemaphoreType.DMA((2, 6)),
            pltpu.VMEM((stored, local_width, 128), BF16),
            pltpu.VMEM((groups, local_width, 128), BF16),
            pltpu.VMEM((groups, local_width, 128), BF16),
            pltpu.VMEM((groups, local_width, 128), BF16),
            pltpu.VMEM((groups, local_width, 128), BF16),
            pltpu.SemaphoreType.DMA((3, groups)),
            pltpu.SemaphoreType.DMA((3, groups)),
            pltpu.SemaphoreType.DMA((2, 5, 6)),
            pltpu.SemaphoreType.DMA((2, 5, 6)),
            pltpu.SemaphoreType.DMA((2, 5, 6)),
            pltpu.SemaphoreType.DMA((2, 5, 6)),
        ]
        + lora_scratch(sizes, cap, local_width)
        + [x for i, x in enumerate(lora_scratch(sizes, cap, local_width)) if i not in (0, 1, 6, 7)],
        compiler_params=pltpu.CompilerParams(
            collective_id=0, has_side_effects=True, vmem_limit_bytes=50 << 20
        ),
        name="layer",
    )(
        small, norm_gain.reshape(width // 128, 128), hidden, query_matrix, adapter_store, kv_pages.reshape(pool * half, lanes), output_weight,
    )


def solution(mesh):
    sizes = (mesh.shape["group"], mesh.shape["tensor"])
    in_specs = (
        P("group", None),
        P(),
        P(None, "tensor"),
        P("tensor", None),
        P("group", "tensor", None, None),
        P("group", None),
        P("group", None),
        P("group", None),
        P("group", "tensor", None),
        P(),
        P(),
    )
    return jax.shard_map(
        functools.partial(body, sizes),
        mesh=mesh,
        in_specs=in_specs,
        out_specs=P("group", None),
        check_vma=False,
    )
```
